128 devices in a mesh: south: 2 (over x_hi), east: 8 (over y, core), down: 8 (over z, x_lo).
Axes of the slice: x: 4 (x_hi: 2, x_lo: 2; x = x_hi * 2 + x_lo), y: 4, z: 4, core: 2. Of those that a mesh axis runs over, the one named last changes fastest.
Arguments:
- field_values: float32 [256, 64, 64, 128], P('south', 'east', 'down'), may hold values from 0.5 to 2
- flow_j: float32 [256, 64, 64, 128], P('south', 'east', 'down'), may hold values from -0.3 to 0.3
- flow_i: float32 [256, 64, 64, 128], P('south', 'east', 'down'), may hold values from -0.3 to 0.3
- flow_k: float32 [256, 64, 64, 128], P('south', 'east', 'down'), may hold values from -0.3 to 0.3
Outputs:
- standardized: float32 [256, 64, 64, 128], P('south', 'east', 'down')
- field_values_end: float32 [256, 64, 64, 128], P('south', 'east', 'down')
The draws below stay inside these ranges and needn't reach their ends.
All inputs are finite; a program needn't handle non-finite values.
Results may differ from the reference program's by a relative error of at most 0.00002.
Values sent between devices are 32-bit elements; how exact they have to be, the bound alone decides.
A program may use at most 128 MiB of HBM per device.

```python
import jax
import jax.numpy as jnp
from jax import lax

GRID_J = 256
GRID_I = 64
GRID_K = 64
LEVELS = 128
STEPS = 6


def block_scale(key, shape, cuts, smallest, high):
    def one(dim, blocks):
        steps = jax.random.uniform(jax.random.fold_in(jax.random.fold_in(key, 6), dim), (blocks,), jnp.float32, smallest / len(cuts), high / len(cuts))
        return jnp.repeat(jnp.exp(steps), shape[dim] // blocks).reshape((-1,) + (1,) * (len(shape) - dim - 1))

    level = one(*cuts[0])
    for cut in cuts[1:]:
        level = level * one(*cut)
    return level


def setup_inputs(seed: int = 0) -> dict:
    key_of = jax.random.split(jax.random.key(seed), 5)
    return {
        "field_values": jnp.clip(0.5 + 1.5 * jax.random.uniform(key_of[0], (GRID_J, GRID_I, GRID_K, LEVELS), jnp.float32) ** block_scale(key_of[0], (GRID_J, GRID_I, GRID_K, LEVELS), ((0, 2), (1, 8), (2, 8)), -0.2, 0.2), 0.5, 2.0),
        "flow_j": jnp.clip(jax.random.uniform(key_of[1], (GRID_J, GRID_I, GRID_K, LEVELS), jnp.float32, -0.3, 0.3) * block_scale(key_of[1], (GRID_J, GRID_I, GRID_K, LEVELS), ((0, 2), (1, 8), (2, 8)), -0.4, 0.0), -0.3, 0.3),
        "flow_i": jnp.clip(jax.random.uniform(key_of[2], (GRID_J, GRID_I, GRID_K, LEVELS), jnp.float32, -0.3, 0.3) * block_scale(key_of[2], (GRID_J, GRID_I, GRID_K, LEVELS), ((0, 2), (1, 8), (2, 8)), -0.4, 0.0), -0.3, 0.3),
        "flow_k": jnp.clip(jax.random.uniform(key_of[3], (GRID_J, GRID_I, GRID_K, LEVELS), jnp.float32, -0.3, 0.3) * block_scale(key_of[3], (GRID_J, GRID_I, GRID_K, LEVELS), ((0, 2), (1, 8), (2, 8)), -0.4, 0.0), -0.3, 0.3),
    }


def inner_cells(values, dims):
    for dim in dims:
        values = lax.slice_in_dim(values, 1, values.shape[dim] - 1, axis=dim)
    return values

def side_cells(values, dim, start, dims):
    others = [other for other in dims if other != dim]
    values = inner_cells(values, others)
    return lax.slice_in_dim(values, start, start + values.shape[dim] - 2, axis=dim)

def advance(padded, flow_j, flow_i, flow_k):
    middle = inner_cells(padded, (0, 1, 2))
    lower = [side_cells(padded, dim, 0, (0, 1, 2)) for dim in (0, 1, 2)]
    upper = [side_cells(padded, dim, 2, (0, 1, 2)) for dim in (0, 1, 2)]
    slopes = [above - below for above, below in zip(upper, lower)]
    smooth_rate = 0.05
    spread = lower[0] + upper[0] + lower[1] + upper[1] + lower[2] + upper[2] - 6.0 * middle
    return middle - flow_j * slopes[0] - flow_i * slopes[1] - flow_k * slopes[2] + smooth_rate * spread

def reference(field_values, flow_j, flow_i, flow_k):
    for step in range(STEPS):
        field_values = advance(jnp.pad(field_values, ((1, 1), (1, 1), (1, 1), (0, 0)), mode='constant'), flow_j, flow_i, flow_k)
    line_mean = lax.optimization_barrier(jnp.mean(field_values, axis=0, keepdims=True))
    centred = field_values - line_mean
    line_variance = lax.optimization_barrier(jnp.mean(centred * centred, axis=0, keepdims=True))
    standardized = centred * lax.rsqrt(line_variance + 0.0001)
    return (standardized, field_values)
```

```python
import functools

import jax
import jax.numpy as jnp
from jax import lax
from jax.experimental import pallas as pl
from jax.experimental.pallas import tpu as pltpu
from jax.sharding import PartitionSpec as P

STEPS = 6
RATE = 0.05
EPS = 1e-4
MESH = pl.DeviceIdType.MESH


def place(p, count):
    half = lax.div(p, 2)
    return jnp.where(lax.rem(p, 2) == 0, half, count - 1 - half)


def kernel(
    sizes, x_hbm, fj_hbm, fi_hbm, fk_hbm, std_hbm, end_hbm,
    field, flows, k_out, k_in, std, stat_out, stat_in,
    load_sem, k_send, k_recv, j_send, j_recv, i_send, i_recv, s_send, s_recv, end_sem, std_sem,
):
    n_j, n_i, n_k, n_lev = sizes
    south, east, down = (lax.axis_index(a) for a in ("south", "east", "down"))
    easts, downs = lax.axis_size("east"), lax.axis_size("down")
    has = {
        "k0": down > 0, "k1": down < downs - 1,
        "i0": east > 0, "i1": east < easts - 1,
    }
    near = {
        "k0": {"down": down - 1}, "k1": {"down": down + 1},
        "i0": {"east": east - 1}, "i1": {"east": east + 1},
        "j": {"south": 1 - south},
    }

    def load(a, p):
        i = place(p, n_i)
        src = (x_hbm, fj_hbm, fi_hbm, fk_hbm)[a].at[:, i]
        dst = field.at[0, i + 1, pl.ds(1, n_j)] if a == 0 else flows.at[a - 1, i]
        return pltpu.make_async_copy(src, dst, load_sem.at[a, p])

    for a in range(4):
        @pl.loop(0, n_i)
        def _(p):
            load(a, p).start()

    barrier = pltpu.get_barrier_semaphore()
    count = 1
    pl.semaphore_signal(barrier, inc=1, device_id=near["j"], device_id_type=MESH)
    for side in ("k0", "k1", "i0", "i1"):
        count = count + has[side].astype(jnp.int32)

        @pl.when(has[side])
        def _():
            pl.semaphore_signal(barrier, inc=1, device_id=near[side], device_id_type=MESH)

    nothing = jnp.zeros((8, n_k, n_lev), jnp.float32)
    for d in range(2):
        @pl.when(jnp.logical_not(has[f"k{d}"]))
        def _():
            @pl.loop(0, 2 * n_i)
            def _(q):
                k_in[lax.div(q, n_i), d, lax.rem(q, n_i)] = jnp.zeros((n_j, n_lev), jnp.float32)

        @pl.when(jnp.logical_not(has[f"i{d}"]))
        def _():
            @pl.loop(0, n_j // 8)
            def _(b):
                for par in range(2):
                    field[par, d * (n_i + 1), pl.ds(1 + b * 8, 8)] = nothing

        @pl.when(south == d)
        def _():
            @pl.loop(0, n_i)
            def _(i):
                for par in range(2):
                    field[par, i + 1, d * (n_j + 1)] = nothing[0]

    def k_copy(par, d, p):
        return pltpu.make_async_remote_copy(
            src_ref=k_out.at[par, d, p], dst_ref=k_in.at[par, 1 - d, p],
            send_sem=k_send.at[par, d, p], recv_sem=k_recv.at[par, 1 - d, p],
            device_id=near[f"k{d}"], device_id_type=MESH,
        )

    def k_arrival(par, d, p):
        return pltpu.make_async_remote_copy(
            src_ref=k_out.at[par, 1 - d, p], dst_ref=k_in.at[par, d, p],
            send_sem=k_send.at[par, 1 - d, p], recv_sem=k_recv.at[par, d, p],
            device_id=near[f"k{d}"], device_id_type=MESH,
        )

    def j_copy(par, p):
        i = place(p, n_i)
        return pltpu.make_async_remote_copy(
            src_ref=field.at[par, i + 1, jnp.where(south == 0, n_j, 1)],
            dst_ref=field.at[par, i + 1, jnp.where(south == 0, 0, n_j + 1)],
            send_sem=j_send.at[par, p], recv_sem=j_recv.at[par, p],
            device_id=near["j"], device_id_type=MESH,
        )

    def i_copy(par, d):
        return pltpu.make_async_remote_copy(
            src_ref=field.at[par, 1 + d * (n_i - 1), pl.ds(1, n_j)],
            dst_ref=field.at[par, (1 - d) * (n_i + 1), pl.ds(1, n_j)],
            send_sem=i_send.at[par, d], recv_sem=i_recv.at[par, 1 - d],
            device_id=near[f"i{d}"], device_id_type=MESH,
        )

    def i_arrival(par, d):
        return pltpu.make_async_remote_copy(
            src_ref=field.at[par, 1 + (1 - d) * (n_i - 1), pl.ds(1, n_j)],
            dst_ref=field.at[par, d * (n_i + 1), pl.ds(1, n_j)],
            send_sem=i_send.at[par, 1 - d], recv_sem=i_recv.at[par, d],
            device_id=near[f"i{d}"], device_id_type=MESH,
        )

    rows = field.reshape(2, n_i + 2, (n_j + 2) * n_k, n_lev)

    def extract(par, p):
        i = place(p, n_i)
        for d in range(2):
            k_out[par, d, p] = rows[par, i + 1, pl.ds(n_k + d * (n_k - 1), n_j, stride=n_k), :]

    def send(par, p):
        for d in range(2):
            @pl.when(has[f"k{d}"])
            def _():
                k_copy(par, d, p).start()
        j_copy(par, p).start()
        for d in range(2):
            @pl.when(jnp.logical_and(p == d, has[f"i{d}"]))
            def _():
                i_copy(par, d).start()

    def sent(par, p):
        for d in range(2):
            @pl.when(has[f"k{d}"])
            def _():
                k_copy(par, d, p).wait_send()
        j_copy(par, p).wait_send()
        for d in range(2):
            @pl.when(jnp.logical_and(p == d, has[f"i{d}"]))
            def _():
                i_copy(par, d).wait_send()

    def arrived(par, p):
        for d in range(2):
            @pl.when(has[f"k{d}"])
            def _():
                k_arrival(par, d, p).wait_recv()
        j_copy(par, p).wait_recv()
        for d in range(2):
            @pl.when(jnp.logical_and(p == d, has[f"i{d}"]))
            def _():
                i_arrival(par, d).wait_recv()

    level = lax.broadcasted_iota(jnp.int32, (n_k, n_lev), 0)
    first, last = level == 0, level == n_k - 1

    def advance(par, i, p, b, u):
        j = b * 8 + u
        mid = field[par, i + 1, j + 1]
        j0, j1 = field[par, i + 1, j], field[par, i + 1, j + 2]
        i0, i1 = field[par, i, j + 1], field[par, i + 2, j + 1]
        k0 = jnp.where(first, jnp.broadcast_to(k_in[par, 0, p, pl.ds(j, 1), :], (n_k, n_lev)), pltpu.roll(mid, 1, 0))
        k1 = jnp.where(last, jnp.broadcast_to(k_in[par, 1, p, pl.ds(j, 1), :], (n_k, n_lev)), pltpu.roll(mid, n_k - 1, 0))
        around = ((j0 + j1) + (i0 + i1)) + (k0 + k1)
        kept = (1.0 - 6.0 * RATE) * mid + RATE * around
        return kept - flows[0, i, j] * (j1 - j0) - flows[1, i, j] * (i1 - i0) - flows[2, i, j] * (k1 - k0)

    @pl.loop(0, n_i)
    def _(p):
        load(0, p).wait()
        extract(0, p)

    pl.semaphore_wait(barrier, count)

    @pl.loop(0, n_i)
    def _(p):
        send(0, p)

    @pl.loop(0, STEPS - 1)
    def _(n):
        par = lax.rem(n, 2)

        @pl.loop(0, n_i)
        def _(p):
            i = place(p, n_i)

            @pl.when(n == 0)
            def _():
                for a in range(1, 4):
                    load(a, p).wait()

            arrived(par, p)

            @pl.when(n > 0)
            def _():
                sent(1 - par, p)

            @pl.loop(0, n_j // 8)
            def _(b):
                for u in range(8):
                    field[1 - par, i + 1, b * 8 + u + 1] = advance(par, i, p, b, u)

            extract(1 - par, p)
            send(1 - par, p)

    par = (STEPS - 1) % 2
    fin = 1 - par

    def stat_copy(p):
        return pltpu.make_async_remote_copy(
            src_ref=stat_out.at[p], dst_ref=stat_in.at[p],
            send_sem=s_send.at[p], recv_sem=s_recv.at[p],
            device_id=near["j"], device_id_type=MESH,
        )

    def end_copy(p):
        i = place(p, n_i)
        return pltpu.make_async_copy(field.at[fin, i + 1, pl.ds(1, n_j)], end_hbm.at[:, i], end_sem.at[p])

    def std_copy(p):
        i = place(p, n_i)
        return pltpu.make_async_copy(std.at[i], std_hbm.at[:, i], std_sem.at[p])

    def finish(p):
        i = place(p, n_i)
        stat_copy(p).wait_recv()
        mine, other = stat_out[p, 0], stat_in[p, 0]
        gap = mine - other
        mean = 0.5 * (mine + other)
        squares = stat_out[p, 1] + stat_in[p, 1] + (0.5 * n_j) * (gap * gap)
        scale = lax.rsqrt(squares * (0.5 / n_j) + EPS)

        @pl.loop(0, n_j // 8)
        def _(b):
            for u in range(8):
                j = b * 8 + u
                std[i, j] = (field[fin, i + 1, j + 1] - mean) * scale

        std_copy(p).start()

    @pl.loop(0, n_i)
    def _(p):
        i = place(p, n_i)
        arrived(par, p)
        sent(fin, p)

        def ahead(b, total):
            parts = []
            for u in range(8):
                new = advance(par, i, p, b, u)
                field[fin, i + 1, b * 8 + u + 1] = new
                parts.append(new)
            while len(parts) > 1:
                parts = [a + c for a, c in zip(parts[::2], parts[1::2])]
            return total + parts[0]

        total = lax.fori_loop(0, n_j // 8, ahead, jnp.zeros((n_k, n_lev), jnp.float32))
        end_copy(p).start()
        mean = total * (1.0 / n_j)

        def spread(b, total):
            parts = []
            for u in range(8):
                off = field[fin, i + 1, b * 8 + u + 1] - mean
                parts.append(off * off)
            while len(parts) > 1:
                parts = [a + c for a, c in zip(parts[::2], parts[1::2])]
            return total + parts[0]

        stat_out[p, 0] = mean
        stat_out[p, 1] = lax.fori_loop(0, n_j // 8, spread, jnp.zeros((n_k, n_lev), jnp.float32))
        stat_copy(p).start()

        @pl.when(p > 0)
        def _():
            finish(p - 1)

    finish(n_i - 1)

    @pl.loop(0, n_i)
    def _(p):
        sent(par, p)
        stat_copy(p).wait_send()
        end_copy(p).wait()
        std_copy(p).wait()


def per_device(field_values, flow_j, flow_i, flow_k):
    n_j, n_i, n_k, n_lev = sizes = field_values.shape
    f32, dma = jnp.float32, pltpu.SemaphoreType.DMA
    out = jax.ShapeDtypeStruct(sizes, f32)
    anywhere = pl.BlockSpec(memory_space=pl.ANY)
    return pl.pallas_call(
        functools.partial(kernel, sizes),
        out_shape=(out, out),
        in_specs=[anywhere] * 4,
        out_specs=(anywhere, anywhere),
        scratch_shapes=[
            pltpu.VMEM((2, n_i + 2, n_j + 2, n_k, n_lev), f32),
            pltpu.VMEM((3, n_i, n_j, n_k, n_lev), f32),
            pltpu.VMEM((2, 2, n_i, n_j, n_lev), f32),
            pltpu.VMEM((2, 2, n_i, n_j, n_lev), f32),
            pltpu.VMEM((n_i, n_j, n_k, n_lev), f32),
            pltpu.VMEM((n_i, 2, n_k, n_lev), f32),
            pltpu.VMEM((n_i, 2, n_k, n_lev), f32),
            dma((4, n_i)),
            dma((2, 2, n_i)), dma((2, 2, n_i)),
            dma((2, n_i)), dma((2, n_i)),
            dma((2, 2)), dma((2, 2)),
            dma((n_i,)), dma((n_i,)),
            dma((n_i,)), dma((n_i,)),
        ],
        compiler_params=pltpu.CompilerParams(
            collective_id=0, has_side_effects=True, vmem_limit_bytes=60 * 1024 * 1024
        ),
        name="transport",
    )(field_values, flow_j, flow_i, flow_k)


def solution(mesh):
    spec = P("south", "east", "down", None)
    return jax.shard_map(
        per_device, mesh=mesh, in_specs=(spec,) * 4, out_specs=(spec, spec), check_vma=False
    )
```

```python
import functools

import jax
import jax.numpy as jnp
from jax import lax
from jax.experimental import pallas as pl
from jax.experimental.pallas import tpu as pltpu
from jax.sharding import PartitionSpec as P

STEPS = 6
RATE = 0.05
EPS = 1e-4
LAG = 1
MESH = pl.DeviceIdType.MESH


def place(p, count):
    half = lax.div(p, 2)
    return jnp.where(lax.rem(p, 2) == 0, half, count - 1 - half)


def kernel(
    sizes, x_hbm, fj_hbm, fi_hbm, fk_hbm, std, end,
    field, flows, k_out, k_in, passing, stat_out, stat_in,
    load_sem, k_send, k_recv, p_send, p_recv, j_send, j_recv, i_send, i_recv, s_send, s_recv,
):
    n_j, n_i, n_k, n_lev = sizes
    south, east, down = (lax.axis_index(a) for a in ("south", "east", "down"))
    easts, downs = lax.axis_size("east"), lax.axis_size("down")
    has = {
        "k0": down > 0, "k1": down < downs - 1,
        "i0": east > 0, "i1": east < easts - 1,
        "p0": down > 1, "p1": down < downs - 2,
    }
    near = {
        "k0": {"down": down - 1}, "k1": {"down": down + 1},
        "i0": {"east": east - 1}, "i1": {"east": east + 1},
        "p0": {"down": down - 2}, "p1": {"down": down + 2},
        "j": {"south": 1 - south},
    }
    odd = lax.rem(down, 2) == 1
    slant = (jnp.logical_and(jnp.logical_not(odd), has["k0"]), jnp.logical_and(odd, has["k1"]))

    def passed(sender, p):
        straight = lax.div(n_i * jnp.where(odd, downs - 1 - sender, sender), downs)
        return lax.div((p + 1) * straight, n_i) == lax.div(p * straight, n_i)

    passer = jnp.where(odd, down > 1, down < downs - 2)
    pass_from = jnp.where(odd, down - 2, down + 2)
    pass_side = jnp.where(odd, 0, 1)

    def pass_copy(n, p):
        par = lax.rem(n, 2)
        return pltpu.make_async_remote_copy(
            src_ref=passing.at[n, p], dst_ref=k_in.at[par, pass_side, p],
            send_sem=p_send.at[par, p], recv_sem=k_recv.at[par, pass_side, p],
            device_id={"down": jnp.where(odd, down - 1, down + 1)}, device_id_type=MESH,
        )

    def pass_arrival(n, p):
        par = lax.rem(n, 2)
        return pltpu.make_async_remote_copy(
            src_ref=k_out.at[par, 0, p], dst_ref=passing.at[n, p],
            send_sem=p_send.at[par, p], recv_sem=p_recv.at[par, p],
            device_id={"down": pass_from}, device_id_type=MESH,
        )

    def pass_on(n, p):
        @pl.when(jnp.logical_and(passer, passed(pass_from, p)))
        def _():
            pass_arrival(n, p).wait_recv()

            @pl.when(n >= 2)
            def _():
                pass_copy(n - 2, p).wait_send()

            pass_copy(n, p).start()

    def load(a, p):
        i = place(p, n_i)
        src = (x_hbm, fj_hbm, fi_hbm, fk_hbm)[a].at[:, i]
        dst = field.at[0, i + 1, pl.ds(1, n_j)] if a == 0 else flows.at[a - 1, i]
        return pltpu.make_async_copy(src, dst, load_sem.at[a, p])

    for a in range(4):
        @pl.loop(0, n_i)
        def _(p):
            load(a, p).start()

    barrier = pltpu.get_barrier_semaphore()
    count = 1
    pl.semaphore_signal(barrier, inc=1, device_id=near["j"], device_id_type=MESH)
    for side in ("k0", "k1", "i0", "i1", "p0", "p1"):
        count = count + has[side].astype(jnp.int32)

        @pl.when(has[side])
        def _():
            pl.semaphore_signal(barrier, inc=1, device_id=near[side], device_id_type=MESH)

    nothing = jnp.zeros((8, n_k, n_lev), jnp.float32)
    for d in range(2):
        @pl.when(jnp.logical_not(has[f"k{d}"]))
        def _():
            @pl.loop(0, 2 * n_i)
            def _(q):
                k_in[lax.div(q, n_i), d, lax.rem(q, n_i)] = jnp.zeros((n_j, n_lev), jnp.float32)

        @pl.when(jnp.logical_not(has[f"i{d}"]))
        def _():
            @pl.loop(0, n_j // 8)
            def _(b):
                for par in range(2):
                    field[par, d * (n_i + 1), pl.ds(1 + b * 8, 8)] = nothing

        @pl.when(south == d)
        def _():
            @pl.loop(0, n_i)
            def _(i):
                for par in range(2):
                    field[par, i + 1, d * (n_j + 1)] = nothing[0]

    def k_copy(par, d, p):
        return pltpu.make_async_remote_copy(
            src_ref=k_out.at[par, d, p], dst_ref=k_in.at[par, 1 - d, p],
            send_sem=k_send.at[par, d, p], recv_sem=k_recv.at[par, 1 - d, p],
            device_id=near[f"k{d}"], device_id_type=MESH,
        )

    def k_slant(n, d, p):
        par = lax.rem(n, 2)
        return pltpu.make_async_remote_copy(
            src_ref=k_out.at[par, d, p], dst_ref=passing.at[n, p],
            send_sem=k_send.at[par, d, p], recv_sem=p_recv.at[par, p],
            device_id=near[f"p{d}"], device_id_type=MESH,
        )

    def k_arrival(par, d, p):
        return pltpu.make_async_remote_copy(
            src_ref=k_out.at[par, 1 - d, p], dst_ref=k_in.at[par, d, p],
            send_sem=k_send.at[par, 1 - d, p], recv_sem=k_recv.at[par, d, p],
            device_id=near[f"k{d}"], device_id_type=MESH,
        )

    def j_copy(par, p):
        i = place(p, n_i)
        return pltpu.make_async_remote_copy(
            src_ref=field.at[par, i + 1, jnp.where(south == 0, n_j, 1)],
            dst_ref=field.at[par, i + 1, jnp.where(south == 0, 0, n_j + 1)],
            send_sem=j_send.at[par, p], recv_sem=j_recv.at[par, p],
            device_id=near["j"], device_id_type=MESH,
        )

    def i_copy(par, d):
        return pltpu.make_async_remote_copy(
            src_ref=field.at[par, 1 + d * (n_i - 1), pl.ds(1, n_j)],
            dst_ref=field.at[par, (1 - d) * (n_i + 1), pl.ds(1, n_j)],
            send_sem=i_send.at[par, d], recv_sem=i_recv.at[par, 1 - d],
            device_id=near[f"i{d}"], device_id_type=MESH,
        )

    def i_arrival(par, d):
        return pltpu.make_async_remote_copy(
            src_ref=field.at[par, 1 + (1 - d) * (n_i - 1), pl.ds(1, n_j)],
            dst_ref=field.at[par, d * (n_i + 1), pl.ds(1, n_j)],
            send_sem=i_send.at[par, 1 - d], recv_sem=i_recv.at[par, d],
            device_id=near[f"i{d}"], device_id_type=MESH,
        )

    rows = field.reshape(2, n_i + 2, (n_j + 2) * n_k, n_lev)

    def extract(par, p):
        i = place(p, n_i)
        for d in range(2):
            k_out[par, d, p] = rows[par, i + 1, pl.ds(n_k + d * (n_k - 1), n_j, stride=n_k), :]

    def send(n, p):
        par = lax.rem(n, 2)
        around = passed(down, p)
        for d in range(2):
            @pl.when(jnp.logical_and(slant[d], around))
            def _():
                k_slant(n, d, p).start()

            @pl.when(jnp.logical_and(has[f"k{d}"], jnp.logical_not(jnp.logical_and(slant[d], around))))
            def _():
                k_copy(par, d, p).start()
        j_copy(par, p).start()
        for d in range(2):
            @pl.when(jnp.logical_and(p == d, has[f"i{d}"]))
            def _():
                i_copy(par, d).start()

    def sent(par, p):
        for d in range(2):
            @pl.when(has[f"k{d}"])
            def _():
                k_copy(par, d, p).wait_send()
        j_copy(par, p).wait_send()
        for d in range(2):
            @pl.when(jnp.logical_and(p == d, has[f"i{d}"]))
            def _():
                i_copy(par, d).wait_send()

    def arrived(par, p):
        for d in range(2):
            @pl.when(has[f"k{d}"])
            def _():
                k_arrival(par, d, p).wait_recv()
        j_copy(par, p).wait_recv()
        for d in range(2):
            @pl.when(jnp.logical_and(p == d, has[f"i{d}"]))
            def _():
                i_arrival(par, d).wait_recv()

    level = lax.broadcasted_iota(jnp.int32, (n_k, n_lev), 0)
    first, last = level == 0, level == n_k - 1

    def advance(par, i, p, b, u):
        j = b * 8 + u
        mid = field[par, i + 1, j + 1]
        j0, j1 = field[par, i + 1, j], field[par, i + 1, j + 2]
        i0, i1 = field[par, i, j + 1], field[par, i + 2, j + 1]
        k0 = jnp.where(first, jnp.broadcast_to(k_in[par, 0, p, pl.ds(j, 1), :], (n_k, n_lev)), pltpu.roll(mid, 1, 0))
        k1 = jnp.where(last, jnp.broadcast_to(k_in[par, 1, p, pl.ds(j, 1), :], (n_k, n_lev)), pltpu.roll(mid, n_k - 1, 0))
        around = ((j0 + j1) + (i0 + i1)) + (k0 + k1)
        kept = (1.0 - 6.0 * RATE) * mid + RATE * around
        return kept - flows[0, i, j] * (j1 - j0) - flows[1, i, j] * (i1 - i0) - flows[2, i, j] * (k1 - k0)

    @pl.loop(0, n_i)
    def _(p):
        load(0, p).wait()
        extract(0, p)

    pl.semaphore_wait(barrier, count)

    @pl.loop(0, n_i)
    def _(p):
        send(0, p)

    @pl.loop(0, n_i - LAG)
    def _(p):
        pass_on(0, p)

    @pl.loop(0, STEPS - 1)
    def _(n):
        par = lax.rem(n, 2)

        @pl.loop(0, n_i)
        def _(p):
            i = place(p, n_i)

            @pl.when(n == 0)
            def _():
                for a in range(1, 4):
                    load(a, p).wait()

            arrived(par, p)

            @pl.when(n > 0)
            def _():
                sent(1 - par, p)

            @pl.loop(0, n_j // 8)
            def _(b):
                for u in range(8):
                    field[1 - par, i + 1, b * 8 + u + 1] = advance(par, i, p, b, u)

            extract(1 - par, p)
            send(n + 1, p)
            at = (n + 1) * n_i + p - LAG
            pass_on(lax.div(at, n_i), lax.rem(at, n_i))

    par = (STEPS - 1) % 2
    fin = 1 - par

    def stat_copy(p):
        return pltpu.make_async_remote_copy(
            src_ref=stat_out.at[p], dst_ref=stat_in.at[p],
            send_sem=s_send.at[p], recv_sem=s_recv.at[p],
            device_id=near["j"], device_id_type=MESH,
        )

    def finish(p):
        i = place(p, n_i)
        stat_copy(p).wait_recv()
        mine, other = stat_out[p, 0], stat_in[p, 0]
        gap = mine - other
        mean = 0.5 * (mine + other)
        squares = stat_out[p, 1] + stat_in[p, 1] + (0.5 * n_j) * (gap * gap)
        scale = lax.rsqrt(squares * (0.5 / n_j) + EPS)

        @pl.loop(0, n_j // 8)
        def _(b):
            for u in range(8):
                j = b * 8 + u
                std[j, i] = (end[j, i] - mean) * scale

    @pl.loop(0, n_i)
    def _(p):
        i = place(p, n_i)

        @pl.when(p < LAG)
        def _():
            pass_on(STEPS - 1, n_i - LAG + p)

        arrived(par, p)
        sent(fin, p)

        def ahead(b, total):
            parts = []
            for u in range(8):
                new = advance(par, i, p, b, u)
                end[b * 8 + u, i] = new
                parts.append(new)
            while len(parts) > 1:
                parts = [a + c for a, c in zip(parts[::2], parts[1::2])]
            return total + parts[0]

        total = lax.fori_loop(0, n_j // 8, ahead, jnp.zeros((n_k, n_lev), jnp.float32))
        mean = total * (1.0 / n_j)

        def spread(b, total):
            parts = []
            for u in range(8):
                off = end[b * 8 + u, i] - mean
                parts.append(off * off)
            while len(parts) > 1:
                parts = [a + c for a, c in zip(parts[::2], parts[1::2])]
            return total + parts[0]

        stat_out[p, 0] = mean
        stat_out[p, 1] = lax.fori_loop(0, n_j // 8, spread, jnp.zeros((n_k, n_lev), jnp.float32))
        stat_copy(p).start()

        @pl.when(p > 0)
        def _():
            finish(p - 1)

    finish(n_i - 1)

    @pl.loop(0, n_i)
    def _(p):
        sent(par, p)

        @pl.when(jnp.logical_and(passer, passed(pass_from, p)))
        def _():
            for n in (STEPS - 2, STEPS - 1):
                pass_copy(n, p).wait_send()

        stat_copy(p).wait_send()


def per_device(field_values, flow_j, flow_i, flow_k):
    n_j, n_i, n_k, n_lev = sizes = field_values.shape
    f32, dma = jnp.float32, pltpu.SemaphoreType.DMA
    out = jax.ShapeDtypeStruct(sizes, f32)
    anywhere = pl.BlockSpec(memory_space=pl.ANY)
    return pl.pallas_call(
        functools.partial(kernel, sizes),
        out_shape=(out, out),
        in_specs=[anywhere] * 4,
        out_specs=(pl.BlockSpec(memory_space=pltpu.VMEM),) * 2,
        scratch_shapes=[
            pltpu.VMEM((2, n_i + 2, n_j + 2, n_k, n_lev), f32),
            pltpu.VMEM((3, n_i, n_j, n_k, n_lev), f32),
            pltpu.VMEM((2, 2, n_i, n_j, n_lev), f32),
            pltpu.VMEM((2, 2, n_i, n_j, n_lev), f32),
            pltpu.VMEM((STEPS, n_i, n_j, n_lev), f32),
            pltpu.VMEM((n_i, 2, n_k, n_lev), f32),
            pltpu.VMEM((n_i, 2, n_k, n_lev), f32),
            dma((4, n_i)),
            dma((2, 2, n_i)), dma((2, 2, n_i)),
            dma((2, n_i)), dma((2, n_i)),
            dma((2, n_i)), dma((2, n_i)),
            dma((2, 2)), dma((2, 2)),
            dma((n_i,)), dma((n_i,)),
        ],
        compiler_params=pltpu.CompilerParams(
            collective_id=0, has_side_effects=True, vmem_limit_bytes=44 * 1024 * 1024
        ),
        name="transport",
    )(field_values, flow_j, flow_i, flow_k)


def solution(mesh):
    spec = P("south", "east", "down", None)
    return jax.shard_map(
        per_device, mesh=mesh, in_specs=(spec,) * 4, out_specs=(spec, spec), check_vma=False
    )
```

```python
import functools

import jax
import jax.numpy as jnp
from jax import lax
from jax.experimental import pallas as pl
from jax.experimental.pallas import tpu as pltpu
from jax.sharding import PartitionSpec as P

STEPS = 6
RATE = 0.05
EPS = 1e-4
LAG = 1
MESH = pl.DeviceIdType.MESH


def place(p, count):
    half = lax.div(p, 2)
    return jnp.where(lax.rem(p, 2) == 0, half, count - 1 - half)


def kernel(
    sizes, x_hbm, fj_hbm, fi_hbm, fk_hbm, std, end,
    field, flows, k_out, k_in, passing, stat_out, stat_in,
    load_sem, k_send, k_recv, p_send, p_recv, j_send, j_recv, i_send, i_recv, s_send, s_recv,
):
    n_j, n_i, n_k, n_lev = sizes
    south, east, down = (lax.axis_index(a) for a in ("south", "east", "down"))
    easts, downs = lax.axis_size("east"), lax.axis_size("down")
    has = {
        "k0": down > 0, "k1": down < downs - 1,
        "i0": east > 0, "i1": east < easts - 1,
        "p0": down > 1, "p1": down < downs - 2,
    }
    near = {
        "k0": {"down": down - 1}, "k1": {"down": down + 1},
        "i0": {"east": east - 1}, "i1": {"east": east + 1},
        "p0": {"down": down - 2}, "p1": {"down": down + 2},
        "j": {"south": 1 - south},
    }
    odd = lax.rem(down, 2) == 1
    slant = (jnp.logical_and(jnp.logical_not(odd), has["k0"]), jnp.logical_and(odd, has["k1"]))

    def passed(sender, p):
        straight = lax.div(n_i * jnp.where(odd, downs - 1 - sender, sender), downs)
        return lax.div((p + 1) * straight, n_i) == lax.div(p * straight, n_i)

    passer = jnp.where(odd, down > 1, down < downs - 2)
    pass_from = jnp.where(odd, down - 2, down + 2)
    pass_side = jnp.where(odd, 0, 1)

    def pass_copy(n, p):
        par = lax.rem(n, 2)
        return pltpu.make_async_remote_copy(
            src_ref=passing.at[n, p], dst_ref=k_in.at[par, pass_side, p],
            send_sem=p_send.at[par, p], recv_sem=k_recv.at[par, pass_side, p],
            device_id={"down": jnp.where(odd, down - 1, down + 1)}, device_id_type=MESH,
        )

    def pass_arrival(n, p):
        par = lax.rem(n, 2)
        return pltpu.make_async_remote_copy(
            src_ref=k_out.at[par, 0, p], dst_ref=passing.at[n, p],
            send_sem=p_send.at[par, p], recv_sem=p_recv.at[par, p],
            device_id={"down": pass_from}, device_id_type=MESH,
        )

    def pass_on(n, p):
        @pl.when(jnp.logical_and(passer, passed(pass_from, p)))
        def _():
            pass_arrival(n, p).wait_recv()

            @pl.when(n >= 2)
            def _():
                pass_copy(n - 2, p).wait_send()

            pass_copy(n, p).start()

    def load(a, p):
        i = place(p, n_i)
        src = (x_hbm, fj_hbm, fi_hbm, fk_hbm)[a].at[:, i]
        dst = field.at[0, i + 1, pl.ds(1, n_j)] if a == 0 else flows.at[a - 1, i]
        return pltpu.make_async_copy(src, dst, load_sem.at[a, p])

    for a in range(4):
        @pl.loop(0, n_i)
        def _(p):
            load(a, p).start()

    barrier = pltpu.get_barrier_semaphore()
    count = 1
    pl.semaphore_signal(barrier, inc=1, device_id=near["j"], device_id_type=MESH)
    for side in ("k0", "k1", "i0", "i1", "p0", "p1"):
        count = count + has[side].astype(jnp.int32)

        @pl.when(has[side])
        def _():
            pl.semaphore_signal(barrier, inc=1, device_id=near[side], device_id_type=MESH)

    nothing = jnp.zeros((8, n_k, n_lev), jnp.float32)
    for d in range(2):
        @pl.when(jnp.logical_not(has[f"k{d}"]))
        def _():
            @pl.loop(0, 2 * n_i)
            def _(q):
                k_in[lax.div(q, n_i), d, lax.rem(q, n_i)] = jnp.zeros((n_j, n_lev), jnp.float32)

        @pl.when(jnp.logical_not(has[f"i{d}"]))
        def _():
            @pl.loop(0, n_j // 8)
            def _(b):
                for par in range(2):
                    field[par, d * (n_i + 1), pl.ds(1 + b * 8, 8)] = nothing

        @pl.when(south == d)
        def _():
            @pl.loop(0, n_i)
            def _(i):
                for par in range(2):
                    field[par, i + 1, d * (n_j + 1)] = nothing[0]

    def k_copy(par, d, p):
        return pltpu.make_async_remote_copy(
            src_ref=k_out.at[par, d, p], dst_ref=k_in.at[par, 1 - d, p],
            send_sem=k_send.at[par, d, p], recv_sem=k_recv.at[par, 1 - d, p],
            device_id=near[f"k{d}"], device_id_type=MESH,
        )

    def k_slant(n, d, p):
        par = lax.rem(n, 2)
        return pltpu.make_async_remote_copy(
            src_ref=k_out.at[par, d, p], dst_ref=passing.at[n, p],
            send_sem=k_send.at[par, d, p], recv_sem=p_recv.at[par, p],
            device_id=near[f"p{d}"], device_id_type=MESH,
        )

    def k_arrival(par, d, p):
        return pltpu.make_async_remote_copy(
            src_ref=k_out.at[par, 1 - d, p], dst_ref=k_in.at[par, d, p],
            send_sem=k_send.at[par, 1 - d, p], recv_sem=k_recv.at[par, d, p],
            device_id=near[f"k{d}"], device_id_type=MESH,
        )

    def j_copy(par, p):
        i = place(p, n_i)
        return pltpu.make_async_remote_copy(
            src_ref=field.at[par, i + 1, jnp.where(south == 0, n_j, 1)],
            dst_ref=field.at[par, i + 1, jnp.where(south == 0, 0, n_j + 1)],
            send_sem=j_send.at[par, p], recv_sem=j_recv.at[par, p],
            device_id=near["j"], device_id_type=MESH,
        )

    def i_copy(par, d):
        return pltpu.make_async_remote_copy(
            src_ref=field.at[par, 1 + d * (n_i - 1), pl.ds(1, n_j)],
            dst_ref=field.at[par, (1 - d) * (n_i + 1), pl.ds(1, n_j)],
            send_sem=i_send.at[par, d], recv_sem=i_recv.at[par, 1 - d],
            device_id=near[f"i{d}"], device_id_type=MESH,
        )

    def i_arrival(par, d):
        return pltpu.make_async_remote_copy(
            src_ref=field.at[par, 1 + (1 - d) * (n_i - 1), pl.ds(1, n_j)],
            dst_ref=field.at[par, d * (n_i + 1), pl.ds(1, n_j)],
            send_sem=i_send.at[par, 1 - d], recv_sem=i_recv.at[par, d],
            device_id=near[f"i{d}"], device_id_type=MESH,
        )

    rows = field.reshape(2, n_i + 2, (n_j + 2) * n_k, n_lev)

    def extract(par, p):
        i = place(p, n_i)
        for d in range(2):
            k_out[par, d, p] = rows[par, i + 1, pl.ds(n_k + d * (n_k - 1), n_j, stride=n_k), :]

    def send(n, p):
        par = lax.rem(n, 2)
        around = passed(down, p)
        for d in range(2):
            @pl.when(jnp.logical_and(slant[d], around))
            def _():
                k_slant(n, d, p).start()

            @pl.when(jnp.logical_and(has[f"k{d}"], jnp.logical_not(jnp.logical_and(slant[d], around))))
            def _():
                k_copy(par, d, p).start()
        j_copy(par, p).start()
        for d in range(2):
            @pl.when(jnp.logical_and(p == d, has[f"i{d}"]))
            def _():
                i_copy(par, d).start()

    def sent(par, p):
        for d in range(2):
            @pl.when(has[f"k{d}"])
            def _():
                k_copy(par, d, p).wait_send()
        j_copy(par, p).wait_send()
        for d in range(2):
            @pl.when(jnp.logical_and(p == d, has[f"i{d}"]))
            def _():
                i_copy(par, d).wait_send()

    def arrived(par, p):
        for d in range(2):
            @pl.when(has[f"k{d}"])
            def _():
                k_arrival(par, d, p).wait_recv()
        j_copy(par, p).wait_recv()
        for d in range(2):
            @pl.when(jnp.logical_and(p == d, has[f"i{d}"]))
            def _():
                i_arrival(par, d).wait_recv()

    level = lax.broadcasted_iota(jnp.int32, (n_k, n_lev), 0)
    first, last = level == 0, level == n_k - 1

    def advance(par, i, p, b, u):
        j = b * 8 + u
        mid = field[par, i + 1, j + 1]
        j0, j1 = field[par, i + 1, j], field[par, i + 1, j + 2]
        i0, i1 = field[par, i, j + 1], field[par, i + 2, j + 1]
        k0 = jnp.where(first, jnp.broadcast_to(k_in[par, 0, p, pl.ds(j, 1), :], (n_k, n_lev)), pltpu.roll(mid, 1, 0))
        k1 = jnp.where(last, jnp.broadcast_to(k_in[par, 1, p, pl.ds(j, 1), :], (n_k, n_lev)), pltpu.roll(mid, n_k - 1, 0))
        around = ((j0 + j1) + (i0 + i1)) + (k0 + k1)
        kept = (1.0 - 6.0 * RATE) * mid + RATE * around
        return kept - flows[0, i, j] * (j1 - j0) - flows[1, i, j] * (i1 - i0) - flows[2, i, j] * (k1 - k0)

    @pl.loop(0, n_i)
    def _(p):
        load(0, p).wait()
        extract(0, p)

    pl.semaphore_wait(barrier, count)

    @pl.loop(0, n_i)
    def _(p):
        send(0, p)

    @pl.loop(0, n_i - LAG)
    def _(p):
        pass_on(0, p)

    @pl.loop(0, STEPS - 1)
    def _(n):
        par = lax.rem(n, 2)

        @pl.loop(0, n_i)
        def _(p):
            i = place(p, n_i)

            @pl.when(n == 0)
            def _():
                for a in range(1, 4):
                    load(a, p).wait()

            arrived(par, p)

            @pl.when(n > 0)
            def _():
                sent(1 - par, p)

            @pl.loop(0, n_j // 8)
            def _(b):
                new = [advance(par, i, p, b, u) for u in range(8)]
                for u in range(8):
                    field[1 - par, i + 1, b * 8 + u + 1] = new[u]

            extract(1 - par, p)
            send(n + 1, p)
            at = (n + 1) * n_i + p - LAG
            pass_on(lax.div(at, n_i), lax.rem(at, n_i))

    par = (STEPS - 1) % 2
    fin = 1 - par

    def stat_copy(p):
        return pltpu.make_async_remote_copy(
            src_ref=stat_out.at[p], dst_ref=stat_in.at[p],
            send_sem=s_send.at[p], recv_sem=s_recv.at[p],
            device_id=near["j"], device_id_type=MESH,
        )

    def finish(p):
        i = place(p, n_i)
        stat_copy(p).wait_recv()
        mine, other = stat_out[p, 0], stat_in[p, 0]
        gap = mine - other
        mean = 0.5 * (mine + other)
        squares = stat_out[p, 1] + stat_in[p, 1] + (0.5 * n_j) * (gap * gap)
        scale = lax.rsqrt(squares * (0.5 / n_j) + EPS)

        @pl.loop(0, n_j // 8)
        def _(b):
            done = [(end[b * 8 + u, i] - mean) * scale for u in range(8)]
            for u in range(8):
                std[b * 8 + u, i] = done[u]

    @pl.loop(0, n_i)
    def _(p):
        i = place(p, n_i)

        @pl.when(p < LAG)
        def _():
            pass_on(STEPS - 1, n_i - LAG + p)

        arrived(par, p)
        sent(fin, p)

        def ahead(b, total):
            parts = [advance(par, i, p, b, u) for u in range(8)]
            for u in range(8):
                end[b * 8 + u, i] = parts[u]
            while len(parts) > 1:
                parts = [a + c for a, c in zip(parts[::2], parts[1::2])]
            return total + parts[0]

        total = lax.fori_loop(0, n_j // 8, ahead, jnp.zeros((n_k, n_lev), jnp.float32))
        mean = total * (1.0 / n_j)

        def spread(b, total):
            parts = []
            for u in range(8):
                off = end[b * 8 + u, i] - mean
                parts.append(off * off)
            while len(parts) > 1:
                parts = [a + c for a, c in zip(parts[::2], parts[1::2])]
            return total + parts[0]

        stat_out[p, 0] = mean
        stat_out[p, 1] = lax.fori_loop(0, n_j // 8, spread, jnp.zeros((n_k, n_lev), jnp.float32))
        stat_copy(p).start()

    @pl.loop(0, n_i)
    def _(p):
        finish(p)

    @pl.loop(0, n_i)
    def _(p):
        sent(par, p)

        @pl.when(jnp.logical_and(passer, passed(pass_from, p)))
        def _():
            for n in (STEPS - 2, STEPS - 1):
                pass_copy(n, p).wait_send()

        stat_copy(p).wait_send()


def per_device(field_values, flow_j, flow_i, flow_k):
    n_j, n_i, n_k, n_lev = sizes = field_values.shape
    f32, dma = jnp.float32, pltpu.SemaphoreType.DMA
    out = jax.ShapeDtypeStruct(sizes, f32)
    anywhere = pl.BlockSpec(memory_space=pl.ANY)
    return pl.pallas_call(
        functools.partial(kernel, sizes),
        out_shape=(out, out),
        in_specs=[anywhere] * 4,
        out_specs=(pl.BlockSpec(memory_space=pltpu.VMEM),) * 2,
        scratch_shapes=[
            pltpu.VMEM((2, n_i + 2, n_j + 2, n_k, n_lev), f32),
            pltpu.VMEM((3, n_i, n_j, n_k, n_lev), f32),
            pltpu.VMEM((2, 2, n_i, n_j, n_lev), f32),
            pltpu.VMEM((2, 2, n_i, n_j, n_lev), f32),
            pltpu.VMEM((STEPS, n_i, n_j, n_lev), f32),
            pltpu.VMEM((n_i, 2, n_k, n_lev), f32),
            pltpu.VMEM((n_i, 2, n_k, n_lev), f32),
            dma((4, n_i)),
            dma((2, 2, n_i)), dma((2, 2, n_i)),
            dma((2, n_i)), dma((2, n_i)),
            dma((2, n_i)), dma((2, n_i)),
            dma((2, 2)), dma((2, 2)),
            dma((n_i,)), dma((n_i,)),
        ],
        compiler_params=pltpu.CompilerParams(
            collective_id=0, has_side_effects=True, vmem_limit_bytes=44 * 1024 * 1024
        ),
        name="transport",
    )(field_values, flow_j, flow_i, flow_k)


def solution(mesh):
    spec = P("south", "east", "down", None)
    return jax.shard_map(
        per_device, mesh=mesh, in_specs=(spec,) * 4, out_specs=(spec, spec), check_vma=False
    )
```

```python
import functools

import jax
import jax.numpy as jnp
from jax import lax
from jax.experimental import pallas as pl
from jax.experimental.pallas import tpu as pltpu
from jax.sharding import PartitionSpec as P

STEPS = 6
RATE = 0.05
EPS = 1e-4
LAG = 1
FIRST_LAG = 2
MESH = pl.DeviceIdType.MESH


def place(p, count):
    half = lax.div(p, 2)
    return jnp.where(lax.rem(p, 2) == 0, half, count - 1 - half)


def kernel(
    sizes, x_hbm, fj_hbm, fi_hbm, fk_hbm, std, end,
    field, flows, k_out, k_in, passing, stat_out, stat_in,
    load_sem, k_send, k_recv, p_send, p_recv, j_send, j_recv, i_send, i_recv, s_send, s_recv,
):
    n_j, n_i, n_k, n_lev = sizes
    south, east, down = (lax.axis_index(a) for a in ("south", "east", "down"))
    easts, downs = lax.axis_size("east"), lax.axis_size("down")
    has = {
        "k0": down > 0, "k1": down < downs - 1,
        "i0": east > 0, "i1": east < easts - 1,
        "p0": down > 1, "p1": down < downs - 2,
    }
    near = {
        "k0": {"down": down - 1}, "k1": {"down": down + 1},
        "i0": {"east": east - 1}, "i1": {"east": east + 1},
        "p0": {"down": down - 2}, "p1": {"down": down + 2},
        "j": {"south": 1 - south},
    }
    odd = lax.rem(down, 2) == 1
    slant = (jnp.logical_and(jnp.logical_not(odd), has["k0"]), jnp.logical_and(odd, has["k1"]))

    def passed(sender, p):
        straight = lax.div(n_i * jnp.where(odd, downs - 1 - sender, sender), downs)
        shift = jnp.where(2 * straight > n_i, n_i - straight, 0)
        return lax.div((p + 1) * straight + shift, n_i) == lax.div(p * straight + shift, n_i)

    passer = jnp.where(odd, down > 1, down < downs - 2)
    pass_from = jnp.where(odd, down - 2, down + 2)
    pass_side = jnp.where(odd, 0, 1)

    def pass_copy(n, p):
        par = lax.rem(n, 2)
        return pltpu.make_async_remote_copy(
            src_ref=passing.at[n, p], dst_ref=k_in.at[par, pass_side, p],
            send_sem=p_send.at[par, p], recv_sem=k_recv.at[par, pass_side, p],
            device_id={"down": jnp.where(odd, down - 1, down + 1)}, device_id_type=MESH,
        )

    def pass_arrival(n, p):
        par = lax.rem(n, 2)
        return pltpu.make_async_remote_copy(
            src_ref=k_out.at[par, 0, p], dst_ref=passing.at[n, p],
            send_sem=p_send.at[par, p], recv_sem=p_recv.at[par, p],
            device_id={"down": pass_from}, device_id_type=MESH,
        )

    def pass_on(n, p):
        @pl.when(jnp.logical_and(passer, passed(pass_from, p)))
        def _():
            pass_arrival(n, p).wait_recv()

            @pl.when(n >= 2)
            def _():
                pass_copy(n - 2, p).wait_send()

            pass_copy(n, p).start()

    def load(a, p):
        i = place(p, n_i)
        src = (x_hbm, fj_hbm, fi_hbm, fk_hbm)[a].at[:, i]
        dst = field.at[0, i + 1, pl.ds(1, n_j)] if a == 0 else flows.at[a - 1, i]
        return pltpu.make_async_copy(src, dst, load_sem.at[a, p])

    for p in range(n_i):
        load(0, p).start()

    barrier = pltpu.get_barrier_semaphore()
    count = 1
    pl.semaphore_signal(barrier, inc=1, device_id=near["j"], device_id_type=MESH)
    for side in ("k0", "k1", "i0", "i1", "p0", "p1"):
        count = count + has[side].astype(jnp.int32)

        @pl.when(has[side])
        def _():
            pl.semaphore_signal(barrier, inc=1, device_id=near[side], device_id_type=MESH)

    def k_copy(par, d, p):
        return pltpu.make_async_remote_copy(
            src_ref=k_out.at[par, d, p], dst_ref=k_in.at[par, 1 - d, p],
            send_sem=k_send.at[par, d, p], recv_sem=k_recv.at[par, 1 - d, p],
            device_id=near[f"k{d}"], device_id_type=MESH,
        )

    def k_slant(n, d, p):
        par = lax.rem(n, 2)
        return pltpu.make_async_remote_copy(
            src_ref=k_out.at[par, d, p], dst_ref=passing.at[n, p],
            send_sem=k_send.at[par, d, p], recv_sem=p_recv.at[par, p],
            device_id=near[f"p{d}"], device_id_type=MESH,
        )

    def k_arrival(par, d, p):
        return pltpu.make_async_remote_copy(
            src_ref=k_out.at[par, 1 - d, p], dst_ref=k_in.at[par, d, p],
            send_sem=k_send.at[par, 1 - d, p], recv_sem=k_recv.at[par, d, p],
            device_id=near[f"k{d}"], device_id_type=MESH,
        )

    def j_copy(par, p):
        i = place(p, n_i)
        return pltpu.make_async_remote_copy(
            src_ref=field.at[par, i + 1, jnp.where(south == 0, n_j, 1)],
            dst_ref=field.at[par, i + 1, jnp.where(south == 0, 0, n_j + 1)],
            send_sem=j_send.at[par, p], recv_sem=j_recv.at[par, p],
            device_id=near["j"], device_id_type=MESH,
        )

    def i_copy(par, d):
        return pltpu.make_async_remote_copy(
            src_ref=field.at[par, 1 + d * (n_i - 1), pl.ds(1, n_j)],
            dst_ref=field.at[par, (1 - d) * (n_i + 1), pl.ds(1, n_j)],
            send_sem=i_send.at[par, d], recv_sem=i_recv.at[par, 1 - d],
            device_id=near[f"i{d}"], device_id_type=MESH,
        )

    def i_arrival(par, d):
        return pltpu.make_async_remote_copy(
            src_ref=field.at[par, 1 + (1 - d) * (n_i - 1), pl.ds(1, n_j)],
            dst_ref=field.at[par, d * (n_i + 1), pl.ds(1, n_j)],
            send_sem=i_send.at[par, 1 - d], recv_sem=i_recv.at[par, d],
            device_id=near[f"i{d}"], device_id_type=MESH,
        )

    rows = field.reshape(2, n_i + 2, (n_j + 2) * n_k, n_lev)

    def extract(par, p):
        i = place(p, n_i)
        for d in range(2):
            k_out[par, d, p] = rows[par, i + 1, pl.ds(n_k + d * (n_k - 1), n_j, stride=n_k), :]

    def send(n, p):
        par = lax.rem(n, 2)
        around = passed(down, p)
        for d in range(2):
            @pl.when(jnp.logical_and(slant[d], around))
            def _():
                k_slant(n, d, p).start()

            @pl.when(jnp.logical_and(has[f"k{d}"], jnp.logical_not(jnp.logical_and(slant[d], around))))
            def _():
                k_copy(par, d, p).start()
        j_copy(par, p).start()
        for d in range(2):
            @pl.when(jnp.logical_and(p == d, has[f"i{d}"]))
            def _():
                i_copy(par, d).start()

    def sent(par, p):
        for d in range(2):
            @pl.when(has[f"k{d}"])
            def _():
                k_copy(par, d, p).wait_send()
        j_copy(par, p).wait_send()
        for d in range(2):
            @pl.when(jnp.logical_and(p == d, has[f"i{d}"]))
            def _():
                i_copy(par, d).wait_send()

    def arrived(par, p):
        for d in range(2):
            @pl.when(has[f"k{d}"])
            def _():
                k_arrival(par, d, p).wait_recv()
        j_copy(par, p).wait_recv()
        for d in range(2):
            @pl.when(jnp.logical_and(p == d, has[f"i{d}"]))
            def _():
                i_arrival(par, d).wait_recv()

    level = lax.broadcasted_iota(jnp.int32, (n_k, n_lev), 0)
    first, last = level == 0, level == n_k - 1

    def advance(par, i, p, b, u):
        j = b * 8 + u
        mid = field[par, i + 1, j + 1]
        j0, j1 = field[par, i + 1, j], field[par, i + 1, j + 2]
        i0, i1 = field[par, i, j + 1], field[par, i + 2, j + 1]
        k0 = jnp.where(first, jnp.broadcast_to(k_in[par, 0, p, pl.ds(j, 1), :], (n_k, n_lev)), pltpu.roll(mid, 1, 0))
        k1 = jnp.where(last, jnp.broadcast_to(k_in[par, 1, p, pl.ds(j, 1), :], (n_k, n_lev)), pltpu.roll(mid, n_k - 1, 0))
        around = ((j0 + j1) + (i0 + i1)) + (k0 + k1)
        kept = (1.0 - 6.0 * RATE) * mid + RATE * around
        return kept - flows[0, i, j] * (j1 - j0) - flows[1, i, j] * (i1 - i0) - flows[2, i, j] * (k1 - k0)

    load(0, 0).wait()
    extract(0, 0)
    pl.semaphore_wait(barrier, count)
    send(0, 0)

    @pl.loop(1, n_i)
    def _(p):
        load(0, p).wait()
        extract(0, p)
        send(0, p)

        @pl.when(p >= FIRST_LAG)
        def _():
            pass_on(0, p - FIRST_LAG)

    @pl.loop(0, n_i)
    def _(p):
        for a in range(1, 4):
            load(a, p).start()

    nothing = jnp.zeros((8, n_k, n_lev), jnp.float32)
    for d in range(2):
        @pl.when(jnp.logical_not(has[f"k{d}"]))
        def _():
            @pl.loop(0, 2 * n_i)
            def _(q):
                k_in[lax.div(q, n_i), d, lax.rem(q, n_i)] = jnp.zeros((n_j, n_lev), jnp.float32)

        @pl.when(jnp.logical_not(has[f"i{d}"]))
        def _():
            @pl.loop(0, n_j // 8)
            def _(b):
                for par in range(2):
                    field[par, d * (n_i + 1), pl.ds(1 + b * 8, 8)] = nothing

        @pl.when(south == d)
        def _():
            @pl.loop(0, n_i)
            def _(i):
                for par in range(2):
                    field[par, i + 1, d * (n_j + 1)] = nothing[0]

    @pl.loop(n_i - FIRST_LAG, n_i - LAG)
    def _(p):
        pass_on(0, p)

    @pl.loop(0, STEPS - 1)
    def _(n):
        par = lax.rem(n, 2)

        @pl.loop(0, n_i)
        def _(p):
            i = place(p, n_i)

            @pl.when(n == 0)
            def _():
                for a in range(1, 4):
                    load(a, p).wait()

            arrived(par, p)

            @pl.when(n > 0)
            def _():
                sent(1 - par, p)

            @pl.loop(0, n_j // 8)
            def _(b):
                new = [advance(par, i, p, b, u) for u in range(8)]
                for u in range(8):
                    field[1 - par, i + 1, b * 8 + u + 1] = new[u]

            extract(1 - par, p)
            send(n + 1, p)
            at = (n + 1) * n_i + p - LAG
            pass_on(lax.div(at, n_i), lax.rem(at, n_i))

    par = (STEPS - 1) % 2
    fin = 1 - par

    def stat_copy(p):
        return pltpu.make_async_remote_copy(
            src_ref=stat_out.at[p], dst_ref=stat_in.at[p],
            send_sem=s_send.at[p], recv_sem=s_recv.at[p],
            device_id=near["j"], device_id_type=MESH,
        )

    def finish(p):
        i = place(p, n_i)
        stat_copy(p).wait_recv()
        mine, other = stat_out[p, 0], stat_in[p, 0]
        gap = mine - other
        mean = 0.5 * (mine + other)
        squares = stat_out[p, 1] + stat_in[p, 1] + (0.5 * n_j) * (gap * gap)
        scale = lax.rsqrt(squares * (0.5 / n_j) + EPS)

        @pl.loop(0, n_j // 8)
        def _(b):
            done = [(end[b * 8 + u, i] - mean) * scale for u in range(8)]
            for u in range(8):
                std[b * 8 + u, i] = done[u]

    @pl.loop(0, n_i)
    def _(p):
        i = place(p, n_i)

        @pl.when(p < LAG)
        def _():
            pass_on(STEPS - 1, n_i - LAG + p)

        arrived(par, p)
        sent(fin, p)

        def ahead(b, total):
            parts = [advance(par, i, p, b, u) for u in range(8)]
            for u in range(8):
                end[b * 8 + u, i] = parts[u]
            while len(parts) > 1:
                parts = [a + c for a, c in zip(parts[::2], parts[1::2])]
            return total + parts[0]

        total = lax.fori_loop(0, n_j // 8, ahead, jnp.zeros((n_k, n_lev), jnp.float32))
        mean = total * (1.0 / n_j)

        def spread(b, total):
            parts = []
            for u in range(8):
                off = end[b * 8 + u, i] - mean
                parts.append(off * off)
            while len(parts) > 1:
                parts = [a + c for a, c in zip(parts[::2], parts[1::2])]
            return total + parts[0]

        stat_out[p, 0] = mean
        stat_out[p, 1] = lax.fori_loop(0, n_j // 8, spread, jnp.zeros((n_k, n_lev), jnp.float32))
        stat_copy(p).start()

    @pl.loop(0, n_i)
    def _(p):
        finish(p)

    @pl.loop(0, n_i)
    def _(p):
        sent(par, p)

        @pl.when(jnp.logical_and(passer, passed(pass_from, p)))
        def _():
            for n in (STEPS - 2, STEPS - 1):
                pass_copy(n, p).wait_send()

        stat_copy(p).wait_send()


def write_out(std, end, std_hbm, end_hbm, sem):
    parts = sem.shape[1]
    size = std.shape[0] // parts
    copies = [
        pltpu.make_async_copy(src.at[pl.ds(b * size, size)], dst.at[pl.ds(b * size, size)], sem.at[a, b])
        for b in range(parts)
        for a, (src, dst) in enumerate(((end, end_hbm), (std, std_hbm)))
    ]
    for copy in copies:
        copy.start()
    for copy in copies:
        copy.wait()


def per_device(field_values, flow_j, flow_i, flow_k):
    n_j, n_i, n_k, n_lev = sizes = field_values.shape
    f32, dma = jnp.float32, pltpu.SemaphoreType.DMA
    out = jax.ShapeDtypeStruct(sizes, f32)
    anywhere = pl.BlockSpec(memory_space=pl.ANY)
    std, end = pl.pallas_call(
        functools.partial(kernel, sizes),
        out_shape=(out, out),
        in_specs=[anywhere] * 4,
        out_specs=(pl.BlockSpec(memory_space=pltpu.VMEM),) * 2,
        scratch_shapes=[
            pltpu.VMEM((2, n_i + 2, n_j + 2, n_k, n_lev), f32),
            pltpu.VMEM((3, n_i, n_j, n_k, n_lev), f32),
            pltpu.VMEM((2, 2, n_i, n_j, n_lev), f32),
            pltpu.VMEM((2, 2, n_i, n_j, n_lev), f32),
            pltpu.VMEM((STEPS, n_i, n_j, n_lev), f32),
            pltpu.VMEM((n_i, 2, n_k, n_lev), f32),
            pltpu.VMEM((n_i, 2, n_k, n_lev), f32),
            dma((4, n_i)),
            dma((2, 2, n_i)), dma((2, 2, n_i)),
            dma((2, n_i)), dma((2, n_i)),
            dma((2, n_i)), dma((2, n_i)),
            dma((2, 2)), dma((2, 2)),
            dma((n_i,)), dma((n_i,)),
        ],
        compiler_params=pltpu.CompilerParams(
            collective_id=0, has_side_effects=True, vmem_limit_bytes=44 * 1024 * 1024
        ),
        name="transport",
    )(field_values, flow_j, flow_i, flow_k)
    return pl.pallas_call(
        write_out,
        out_shape=(out, out),
        in_specs=[pl.BlockSpec(memory_space=pltpu.VMEM)] * 2,
        out_specs=(anywhere, anywhere),
        scratch_shapes=[dma((2, 4))],
        compiler_params=pltpu.CompilerParams(vmem_limit_bytes=1024 * 1024),
        name="write_out",
    )(std, end)


def solution(mesh):
    spec = P("south", "east", "down", None)
    return jax.shard_map(
        per_device, mesh=mesh, in_specs=(spec,) * 4, out_specs=(spec, spec), check_vma=False
    )
```

```python
import functools

import jax
import jax.numpy as jnp
from jax import lax
from jax.experimental import pallas as pl
from jax.experimental.pallas import tpu as pltpu
from jax.sharding import PartitionSpec as P

STEPS = 6
RATE = 0.05
EPS = 1e-4
LAG = 1
FIRST_LAG = 2
MESH = pl.DeviceIdType.MESH


def place(p, count):
    half = lax.div(p, 2)
    return jnp.where(lax.rem(p, 2) == 0, half, count - 1 - half)


def kernel(
    sizes, x_hbm, fj_hbm, fi_hbm, fk_hbm, std, end,
    field, flows, k_out, k_in, passing, stat_out, stat_in,
    load_sem, k_send, k_recv, p_send, p_recv, j_send, j_recv, i_send, i_recv, s_send, s_recv,
):
    n_j, n_i, n_k, n_lev = sizes
    south, east, down = (lax.axis_index(a) for a in ("south", "east", "down"))
    easts, downs = lax.axis_size("east"), lax.axis_size("down")
    has = {
        "k0": down > 0, "k1": down < downs - 1,
        "i0": east > 0, "i1": east < easts - 1,
        "p0": down > 1, "p1": down < downs - 2,
    }
    near = {
        "k0": {"down": down - 1}, "k1": {"down": down + 1},
        "i0": {"east": east - 1}, "i1": {"east": east + 1},
        "p0": {"down": down - 2}, "p1": {"down": down + 2},
        "j": {"south": 1 - south},
    }
    odd = lax.rem(down, 2) == 1
    slant = (jnp.logical_and(jnp.logical_not(odd), has["k0"]), jnp.logical_and(odd, has["k1"]))

    def passed(sender, p):
        straight = lax.div(n_i * jnp.where(odd, downs - 1 - sender, sender), downs)
        shift = jnp.where(2 * straight > n_i, n_i - straight, 0)
        return lax.div((p + 1) * straight + shift, n_i) == lax.div(p * straight + shift, n_i)

    passer = jnp.where(odd, down > 1, down < downs - 2)
    pass_from = jnp.where(odd, down - 2, down + 2)
    pass_side = jnp.where(odd, 0, 1)

    def pass_copy(n, p):
        par = lax.rem(n, 2)
        return pltpu.make_async_remote_copy(
            src_ref=passing.at[n, p], dst_ref=k_in.at[par, pass_side, p],
            send_sem=p_send.at[par, p], recv_sem=k_recv.at[par, pass_side, p],
            device_id={"down": jnp.where(odd, down - 1, down + 1)}, device_id_type=MESH,
        )

    def pass_arrival(n, p):
        par = lax.rem(n, 2)
        return pltpu.make_async_remote_copy(
            src_ref=k_out.at[par, 0, p], dst_ref=passing.at[n, p],
            send_sem=p_send.at[par, p], recv_sem=p_recv.at[par, p],
            device_id={"down": pass_from}, device_id_type=MESH,
        )

    def pass_on(n, p):
        @pl.when(jnp.logical_and(passer, passed(pass_from, p)))
        def _():
            pass_arrival(n, p).wait_recv()

            @pl.when(n >= 2)
            def _():
                pass_copy(n - 2, p).wait_send()

            pass_copy(n, p).start()

    def load(a, p):
        i = place(p, n_i)
        src = (x_hbm, fj_hbm, fi_hbm, fk_hbm)[a].at[:, i]
        dst = field.at[0, i + 1, pl.ds(1, n_j)] if a == 0 else flows.at[a - 1, i]
        return pltpu.make_async_copy(src, dst, load_sem.at[a, p])

    for p in range(n_i):
        load(0, p).start()

    barrier = pltpu.get_barrier_semaphore()
    count = 1
    pl.semaphore_signal(barrier, inc=1, device_id=near["j"], device_id_type=MESH)
    for side in ("k0", "k1", "i0", "i1", "p0", "p1"):
        count = count + has[side].astype(jnp.int32)

        @pl.when(has[side])
        def _():
            pl.semaphore_signal(barrier, inc=1, device_id=near[side], device_id_type=MESH)

    def k_copy(par, d, p):
        return pltpu.make_async_remote_copy(
            src_ref=k_out.at[par, d, p], dst_ref=k_in.at[par, 1 - d, p],
            send_sem=k_send.at[par, d, p], recv_sem=k_recv.at[par, 1 - d, p],
            device_id=near[f"k{d}"], device_id_type=MESH,
        )

    def k_slant(n, d, p):
        par = lax.rem(n, 2)
        return pltpu.make_async_remote_copy(
            src_ref=k_out.at[par, d, p], dst_ref=passing.at[n, p],
            send_sem=k_send.at[par, d, p], recv_sem=p_recv.at[par, p],
            device_id=near[f"p{d}"], device_id_type=MESH,
        )

    def k_arrival(par, d, p):
        return pltpu.make_async_remote_copy(
            src_ref=k_out.at[par, 1 - d, p], dst_ref=k_in.at[par, d, p],
            send_sem=k_send.at[par, 1 - d, p], recv_sem=k_recv.at[par, d, p],
            device_id=near[f"k{d}"], device_id_type=MESH,
        )

    def j_copy(par, p):
        i = place(p, n_i)
        return pltpu.make_async_remote_copy(
            src_ref=field.at[par, i + 1, jnp.where(south == 0, n_j, 1)],
            dst_ref=field.at[par, i + 1, jnp.where(south == 0, 0, n_j + 1)],
            send_sem=j_send.at[par, p], recv_sem=j_recv.at[par, p],
            device_id=near["j"], device_id_type=MESH,
        )

    def i_copy(par, d):
        return pltpu.make_async_remote_copy(
            src_ref=field.at[par, 1 + d * (n_i - 1), pl.ds(1, n_j)],
            dst_ref=field.at[par, (1 - d) * (n_i + 1), pl.ds(1, n_j)],
            send_sem=i_send.at[par, d], recv_sem=i_recv.at[par, 1 - d],
            device_id=near[f"i{d}"], device_id_type=MESH,
        )

    def i_arrival(par, d):
        return pltpu.make_async_remote_copy(
            src_ref=field.at[par, 1 + (1 - d) * (n_i - 1), pl.ds(1, n_j)],
            dst_ref=field.at[par, d * (n_i + 1), pl.ds(1, n_j)],
            send_sem=i_send.at[par, 1 - d], recv_sem=i_recv.at[par, d],
            device_id=near[f"i{d}"], device_id_type=MESH,
        )

    rows = field.reshape(2, n_i + 2, (n_j + 2) * n_k, n_lev)

    def extract(par, p):
        i = place(p, n_i)
        for d in range(2):
            k_out[par, d, p] = rows[par, i + 1, pl.ds(n_k + d * (n_k - 1), n_j, stride=n_k), :]

    def send(n, p):
        par = lax.rem(n, 2)
        around = passed(down, p)
        for d in range(2):
            @pl.when(jnp.logical_and(slant[d], around))
            def _():
                k_slant(n, d, p).start()

        for d in range(2):
            @pl.when(jnp.logical_and(has[f"k{d}"], jnp.logical_not(jnp.logical_and(slant[d], around))))
            def _():
                k_copy(par, d, p).start()
        j_copy(par, p).start()
        for d in range(2):
            @pl.when(jnp.logical_and(p == d, has[f"i{d}"]))
            def _():
                i_copy(par, d).start()

    def sent(par, p):
        for d in range(2):
            @pl.when(has[f"k{d}"])
            def _():
                k_copy(par, d, p).wait_send()
        j_copy(par, p).wait_send()
        for d in range(2):
            @pl.when(jnp.logical_and(p == d, has[f"i{d}"]))
            def _():
                i_copy(par, d).wait_send()

    def arrived(par, p):
        for d in range(2):
            @pl.when(has[f"k{d}"])
            def _():
                k_arrival(par, d, p).wait_recv()
        j_copy(par, p).wait_recv()
        for d in range(2):
            @pl.when(jnp.logical_and(p == d, has[f"i{d}"]))
            def _():
                i_arrival(par, d).wait_recv()

    level = lax.broadcasted_iota(jnp.int32, (n_k, n_lev), 0)
    first, last = level == 0, level == n_k - 1

    def advance(par, i, p, b, u):
        j = b * 8 + u
        mid = field[par, i + 1, j + 1]
        j0, j1 = field[par, i + 1, j], field[par, i + 1, j + 2]
        i0, i1 = field[par, i, j + 1], field[par, i + 2, j + 1]
        k0 = jnp.where(first, jnp.broadcast_to(k_in[par, 0, p, pl.ds(j, 1), :], (n_k, n_lev)), pltpu.roll(mid, 1, 0))
        k1 = jnp.where(last, jnp.broadcast_to(k_in[par, 1, p, pl.ds(j, 1), :], (n_k, n_lev)), pltpu.roll(mid, n_k - 1, 0))
        around = ((j0 + j1) + (i0 + i1)) + (k0 + k1)
        kept = (1.0 - 6.0 * RATE) * mid + RATE * around
        return kept - flows[0, i, j] * (j1 - j0) - flows[1, i, j] * (i1 - i0) - flows[2, i, j] * (k1 - k0)

    load(0, 0).wait()
    extract(0, 0)
    pl.semaphore_wait(barrier, count)
    send(0, 0)

    @pl.loop(1, n_i)
    def _(p):
        load(0, p).wait()
        extract(0, p)
        send(0, p)

        @pl.when(p >= FIRST_LAG)
        def _():
            pass_on(0, p - FIRST_LAG)

    @pl.loop(0, n_i)
    def _(p):
        for a in range(1, 4):
            load(a, p).start()

    nothing = jnp.zeros((8, n_k, n_lev), jnp.float32)
    for d in range(2):
        @pl.when(jnp.logical_not(has[f"k{d}"]))
        def _():
            @pl.loop(0, 2 * n_i)
            def _(q):
                k_in[lax.div(q, n_i), d, lax.rem(q, n_i)] = jnp.zeros((n_j, n_lev), jnp.float32)

        @pl.when(jnp.logical_not(has[f"i{d}"]))
        def _():
            @pl.loop(0, n_j // 8)
            def _(b):
                for par in range(2):
                    field[par, d * (n_i + 1), pl.ds(1 + b * 8, 8)] = nothing

        @pl.when(south == d)
        def _():
            @pl.loop(0, n_i)
            def _(i):
                for par in range(2):
                    field[par, i + 1, d * (n_j + 1)] = nothing[0]

    @pl.loop(n_i - FIRST_LAG, n_i - LAG)
    def _(p):
        pass_on(0, p)

    @pl.loop(0, STEPS - 1)
    def _(n):
        par = lax.rem(n, 2)

        @pl.loop(0, n_i)
        def _(p):
            i = place(p, n_i)

            @pl.when(n == 0)
            def _():
                for a in range(1, 4):
                    load(a, p).wait()

            arrived(par, p)

            @pl.when(n > 0)
            def _():
                sent(1 - par, p)

            @pl.loop(0, n_j // 8)
            def _(b):
                new = [advance(par, i, p, b, u) for u in range(8)]
                for u in range(8):
                    field[1 - par, i + 1, b * 8 + u + 1] = new[u]

            extract(1 - par, p)
            at = (n + 1) * n_i + p - LAG
            pass_on(lax.div(at, n_i), lax.rem(at, n_i))
            send(n + 1, p)

    par = (STEPS - 1) % 2
    fin = 1 - par

    def stat_copy(p):
        return pltpu.make_async_remote_copy(
            src_ref=stat_out.at[p], dst_ref=stat_in.at[p],
            send_sem=s_send.at[p], recv_sem=s_recv.at[p],
            device_id=near["j"], device_id_type=MESH,
        )

    def finish(p):
        i = place(p, n_i)
        stat_copy(p).wait_recv()
        mine, other = stat_out[p, 0], stat_in[p, 0]
        gap = mine - other
        mean = 0.5 * (mine + other)
        squares = stat_out[p, 1] + stat_in[p, 1] + (0.5 * n_j) * (gap * gap)
        scale = lax.rsqrt(squares * (0.5 / n_j) + EPS)

        @pl.loop(0, n_j // 8)
        def _(b):
            done = [(end[b * 8 + u, i] - mean) * scale for u in range(8)]
            for u in range(8):
                std[b * 8 + u, i] = done[u]

    @pl.loop(0, n_i)
    def _(p):
        i = place(p, n_i)

        @pl.when(p < LAG)
        def _():
            pass_on(STEPS - 1, n_i - LAG + p)

        arrived(par, p)
        sent(fin, p)

        def ahead(b, total):
            parts = [advance(par, i, p, b, u) for u in range(8)]
            for u in range(8):
                end[b * 8 + u, i] = parts[u]
            while len(parts) > 1:
                parts = [a + c for a, c in zip(parts[::2], parts[1::2])]
            return total + parts[0]

        total = lax.fori_loop(0, n_j // 8, ahead, jnp.zeros((n_k, n_lev), jnp.float32))
        mean = total * (1.0 / n_j)

        def spread(b, total):
            parts = []
            for u in range(8):
                off = end[b * 8 + u, i] - mean
                parts.append(off * off)
            while len(parts) > 1:
                parts = [a + c for a, c in zip(parts[::2], parts[1::2])]
            return total + parts[0]

        stat_out[p, 0] = mean
        stat_out[p, 1] = lax.fori_loop(0, n_j // 8, spread, jnp.zeros((n_k, n_lev), jnp.float32))
        stat_copy(p).start()

    @pl.loop(0, n_i)
    def _(p):
        finish(p)

    @pl.loop(0, n_i)
    def _(p):
        sent(par, p)

        @pl.when(jnp.logical_and(passer, passed(pass_from, p)))
        def _():
            for n in (STEPS - 2, STEPS - 1):
                pass_copy(n, p).wait_send()

        stat_copy(p).wait_send()


def write_out(std, end, std_hbm, end_hbm, sem):
    parts = sem.shape[1]
    size = std.shape[0] // parts
    copies = [
        pltpu.make_async_copy(src.at[pl.ds(b * size, size)], dst.at[pl.ds(b * size, size)], sem.at[a, b])
        for b in range(parts)
        for a, (src, dst) in enumerate(((end, end_hbm), (std, std_hbm)))
    ]
    for copy in copies:
        copy.start()
    for copy in copies:
        copy.wait()


def per_device(field_values, flow_j, flow_i, flow_k):
    n_j, n_i, n_k, n_lev = sizes = field_values.shape
    f32, dma = jnp.float32, pltpu.SemaphoreType.DMA
    out = jax.ShapeDtypeStruct(sizes, f32)
    anywhere = pl.BlockSpec(memory_space=pl.ANY)
    std, end = pl.pallas_call(
        functools.partial(kernel, sizes),
        out_shape=(out, out),
        in_specs=[anywhere] * 4,
        out_specs=(pl.BlockSpec(memory_space=pltpu.VMEM),) * 2,
        scratch_shapes=[
            pltpu.VMEM((2, n_i + 2, n_j + 2, n_k, n_lev), f32),
            pltpu.VMEM((3, n_i, n_j, n_k, n_lev), f32),
            pltpu.VMEM((2, 2, n_i, n_j, n_lev), f32),
            pltpu.VMEM((2, 2, n_i, n_j, n_lev), f32),
            pltpu.VMEM((STEPS, n_i, n_j, n_lev), f32),
            pltpu.VMEM((n_i, 2, n_k, n_lev), f32),
            pltpu.VMEM((n_i, 2, n_k, n_lev), f32),
            dma((4, n_i)),
            dma((2, 2, n_i)), dma((2, 2, n_i)),
            dma((2, n_i)), dma((2, n_i)),
            dma((2, n_i)), dma((2, n_i)),
            dma((2, 2)), dma((2, 2)),
            dma((n_i,)), dma((n_i,)),
        ],
        compiler_params=pltpu.CompilerParams(
            collective_id=0, has_side_effects=True, vmem_limit_bytes=44 * 1024 * 1024
        ),
        name="transport",
    )(field_values, flow_j, flow_i, flow_k)
    return pl.pallas_call(
        write_out,
        out_shape=(out, out),
        in_specs=[pl.BlockSpec(memory_space=pltpu.VMEM)] * 2,
        out_specs=(anywhere, anywhere),
        scratch_shapes=[dma((2, 4))],
        compiler_params=pltpu.CompilerParams(vmem_limit_bytes=1024 * 1024),
        name="write_out",
    )(std, end)


def solution(mesh):
    spec = P("south", "east", "down", None)
    return jax.shard_map(
        per_device, mesh=mesh, in_specs=(spec,) * 4, out_specs=(spec, spec), check_vma=False
    )
```

```python
import functools

import jax
import jax.numpy as jnp
from jax import lax
from jax.experimental import pallas as pl
from jax.experimental.pallas import tpu as pltpu
from jax.sharding import PartitionSpec as P

STEPS = 6
RATE = 0.05
EPS = 1e-4
LAG = 1
FIRST_LAG = 2
MESH = pl.DeviceIdType.MESH


def place(p, count):
    half = lax.div(p, 2)
    return jnp.where(lax.rem(p, 2) == 0, half, count - 1 - half)


def kernel(
    sizes, x_hbm, fj_hbm, fi_hbm, fk_hbm, std, end,
    field, flows, k_out, k_in, passing, stat_out, stat_in,
    load_sem, k_send, k_recv, p_send, p_recv, j_send, j_recv, i_send, i_recv, s_send, s_recv,
):
    n_j, n_i, n_k, n_lev = sizes
    south, east, down = (lax.axis_index(a) for a in ("south", "east", "down"))
    easts, downs = lax.axis_size("east"), lax.axis_size("down")
    has = {
        "k0": down > 0, "k1": down < downs - 1,
        "i0": east > 0, "i1": east < easts - 1,
        "p0": down > 1, "p1": down < downs - 2,
    }
    near = {
        "k0": {"down": down - 1}, "k1": {"down": down + 1},
        "i0": {"east": east - 1}, "i1": {"east": east + 1},
        "p0": {"down": down - 2}, "p1": {"down": down + 2},
        "j": {"south": 1 - south},
    }
    odd = lax.rem(down, 2) == 1
    slant = (jnp.logical_and(jnp.logical_not(odd), has["k0"]), jnp.logical_and(odd, has["k1"]))

    def passed(sender, p):
        straight = lax.div(n_i * jnp.where(odd, downs - 1 - sender, sender), downs)
        shift = jnp.where(2 * straight > n_i, n_i - straight, 0)
        return lax.div((p + 1) * straight + shift, n_i) == lax.div(p * straight + shift, n_i)

    passer = jnp.where(odd, down > 1, down < downs - 2)
    pass_from = jnp.where(odd, down - 2, down + 2)
    pass_side = jnp.where(odd, 0, 1)

    def pass_copy(n, p):
        par = lax.rem(n, 2)
        return pltpu.make_async_remote_copy(
            src_ref=passing.at[n, p], dst_ref=k_in.at[par, pass_side, p],
            send_sem=p_send.at[par, p], recv_sem=k_recv.at[par, pass_side, p],
            device_id={"down": jnp.where(odd, down - 1, down + 1)}, device_id_type=MESH,
        )

    def pass_arrival(n, p):
        par = lax.rem(n, 2)
        return pltpu.make_async_remote_copy(
            src_ref=k_out.at[par, 0, p], dst_ref=passing.at[n, p],
            send_sem=p_send.at[par, p], recv_sem=p_recv.at[par, p],
            device_id={"down": pass_from}, device_id_type=MESH,
        )

    def pass_on(n, p):
        @pl.when(jnp.logical_and(passer, passed(pass_from, p)))
        def _():
            pass_arrival(n, p).wait_recv()

            @pl.when(n >= 2)
            def _():
                pass_copy(n - 2, p).wait_send()

            pass_copy(n, p).start()

    def load(a, p):
        i = place(p, n_i)
        src = (x_hbm, fj_hbm, fi_hbm, fk_hbm)[a].at[:, i]
        dst = field.at[0, i + 1, pl.ds(1, n_j)] if a == 0 else flows.at[a - 1, i]
        return pltpu.make_async_copy(src, dst, load_sem.at[a, p])

    for p in range(n_i):
        load(0, p).start()

    barrier = pltpu.get_barrier_semaphore()
    count = 1
    pl.semaphore_signal(barrier, inc=1, device_id=near["j"], device_id_type=MESH)
    for side in ("k0", "k1", "i0", "i1", "p0", "p1"):
        count = count + has[side].astype(jnp.int32)

        @pl.when(has[side])
        def _():
            pl.semaphore_signal(barrier, inc=1, device_id=near[side], device_id_type=MESH)

    def k_copy(par, d, p):
        return pltpu.make_async_remote_copy(
            src_ref=k_out.at[par, d, p], dst_ref=k_in.at[par, 1 - d, p],
            send_sem=k_send.at[par, d, p], recv_sem=k_recv.at[par, 1 - d, p],
            device_id=near[f"k{d}"], device_id_type=MESH,
        )

    def k_slant(n, d, p):
        par = lax.rem(n, 2)
        return pltpu.make_async_remote_copy(
            src_ref=k_out.at[par, d, p], dst_ref=passing.at[n, p],
            send_sem=k_send.at[par, d, p], recv_sem=p_recv.at[par, p],
            device_id=near[f"p{d}"], device_id_type=MESH,
        )

    def k_arrival(par, d, p):
        return pltpu.make_async_remote_copy(
            src_ref=k_out.at[par, 1 - d, p], dst_ref=k_in.at[par, d, p],
            send_sem=k_send.at[par, 1 - d, p], recv_sem=k_recv.at[par, d, p],
            device_id=near[f"k{d}"], device_id_type=MESH,
        )

    def j_copy(par, p):
        i = place(p, n_i)
        return pltpu.make_async_remote_copy(
            src_ref=field.at[par, i + 1, jnp.where(south == 0, n_j, 1)],
            dst_ref=field.at[par, i + 1, jnp.where(south == 0, 0, n_j + 1)],
            send_sem=j_send.at[par, p], recv_sem=j_recv.at[par, p],
            device_id=near["j"], device_id_type=MESH,
        )

    def i_copy(par, d):
        return pltpu.make_async_remote_copy(
            src_ref=field.at[par, 1 + d * (n_i - 1), pl.ds(1, n_j)],
            dst_ref=field.at[par, (1 - d) * (n_i + 1), pl.ds(1, n_j)],
            send_sem=i_send.at[par, d], recv_sem=i_recv.at[par, 1 - d],
            device_id=near[f"i{d}"], device_id_type=MESH,
        )

    def i_arrival(par, d):
        return pltpu.make_async_remote_copy(
            src_ref=field.at[par, 1 + (1 - d) * (n_i - 1), pl.ds(1, n_j)],
            dst_ref=field.at[par, d * (n_i + 1), pl.ds(1, n_j)],
            send_sem=i_send.at[par, 1 - d], recv_sem=i_recv.at[par, d],
            device_id=near[f"i{d}"], device_id_type=MESH,
        )

    rows = field.reshape(2, n_i + 2, (n_j + 2) * n_k, n_lev)

    def extract(par, p):
        i = place(p, n_i)
        for d in range(2):
            k_out[par, d, p] = rows[par, i + 1, pl.ds(n_k + d * (n_k - 1), n_j, stride=n_k), :]

    def send(n, p):
        par = lax.rem(n, 2)
        around = passed(down, p)
        for d in range(2):
            @pl.when(jnp.logical_and(slant[d], around))
            def _():
                k_slant(n, d, p).start()

        for d in range(2):
            @pl.when(jnp.logical_and(has[f"k{d}"], jnp.logical_not(jnp.logical_and(slant[d], around))))
            def _():
                k_copy(par, d, p).start()
        j_copy(par, p).start()
        for d in range(2):
            @pl.when(jnp.logical_and(p == d, has[f"i{d}"]))
            def _():
                i_copy(par, d).start()

    def sent(par, p):
        for d in range(2):
            @pl.when(has[f"k{d}"])
            def _():
                k_copy(par, d, p).wait_send()
        j_copy(par, p).wait_send()
        for d in range(2):
            @pl.when(jnp.logical_and(p == d, has[f"i{d}"]))
            def _():
                i_copy(par, d).wait_send()

    def arrived(par, p):
        for d in range(2):
            @pl.when(has[f"k{d}"])
            def _():
                k_arrival(par, d, p).wait_recv()
        j_copy(par, p).wait_recv()
        for d in range(2):
            @pl.when(jnp.logical_and(p == d, has[f"i{d}"]))
            def _():
                i_arrival(par, d).wait_recv()

    level = lax.broadcasted_iota(jnp.int32, (n_k, n_lev), 0)
    first, last = level == 0, level == n_k - 1

    def advance(par, i, p, b, u):
        j = b * 8 + u
        mid = field[par, i + 1, j + 1]
        j0, j1 = field[par, i + 1, j], field[par, i + 1, j + 2]
        i0, i1 = field[par, i, j + 1], field[par, i + 2, j + 1]
        k0 = jnp.where(first, jnp.broadcast_to(k_in[par, 0, p, pl.ds(j, 1), :], (n_k, n_lev)), pltpu.roll(mid, 1, 0))
        k1 = jnp.where(last, jnp.broadcast_to(k_in[par, 1, p, pl.ds(j, 1), :], (n_k, n_lev)), pltpu.roll(mid, n_k - 1, 0))
        around = ((j0 + j1) + (i0 + i1)) + (k0 + k1)
        kept = (1.0 - 6.0 * RATE) * mid + RATE * around
        return kept - flows[0, i, j] * (j1 - j0) - flows[1, i, j] * (i1 - i0) - flows[2, i, j] * (k1 - k0)

    load(0, 0).wait()
    extract(0, 0)
    pl.semaphore_wait(barrier, count)
    send(0, 0)

    @pl.loop(1, n_i)
    def _(p):
        load(0, p).wait()
        extract(0, p)
        send(0, p)

        @pl.when(p >= FIRST_LAG)
        def _():
            pass_on(0, p - FIRST_LAG)

    @pl.loop(0, n_i)
    def _(p):
        for a in range(1, 4):
            load(a, p).start()

    nothing = jnp.zeros((8, n_k, n_lev), jnp.float32)
    for d in range(2):
        @pl.when(jnp.logical_not(has[f"k{d}"]))
        def _():
            @pl.loop(0, 2 * n_i)
            def _(q):
                k_in[lax.div(q, n_i), d, lax.rem(q, n_i)] = jnp.zeros((n_j, n_lev), jnp.float32)

        @pl.when(jnp.logical_not(has[f"i{d}"]))
        def _():
            @pl.loop(0, n_j // 8)
            def _(b):
                for par in range(2):
                    field[par, d * (n_i + 1), pl.ds(1 + b * 8, 8)] = nothing

        @pl.when(south == d)
        def _():
            @pl.loop(0, n_i)
            def _(i):
                for par in range(2):
                    field[par, i + 1, d * (n_j + 1)] = nothing[0]

    @pl.loop(n_i - FIRST_LAG, n_i - LAG)
    def _(p):
        pass_on(0, p)

    @pl.loop(0, STEPS - 1)
    def _(n):
        par = lax.rem(n, 2)

        @pl.loop(0, n_i)
        def _(p):
            i = place(p, n_i)

            @pl.when(n == 0)
            def _():
                for a in range(1, 4):
                    load(a, p).wait()

            at = (n + 1) * n_i + p - LAG
            pass_on(lax.div(at, n_i), lax.rem(at, n_i))
            arrived(par, p)

            @pl.when(n > 0)
            def _():
                sent(1 - par, p)

            @pl.loop(0, n_j // 8)
            def _(b):
                new = [advance(par, i, p, b, u) for u in range(8)]
                for u in range(8):
                    field[1 - par, i + 1, b * 8 + u + 1] = new[u]

            extract(1 - par, p)
            send(n + 1, p)

    par = (STEPS - 1) % 2
    fin = 1 - par

    def stat_copy(p):
        return pltpu.make_async_remote_copy(
            src_ref=stat_out.at[p], dst_ref=stat_in.at[p],
            send_sem=s_send.at[p], recv_sem=s_recv.at[p],
            device_id=near["j"], device_id_type=MESH,
        )

    def finish(p):
        i = place(p, n_i)
        stat_copy(p).wait_recv()
        mine, other = stat_out[p, 0], stat_in[p, 0]
        gap = mine - other
        mean = 0.5 * (mine + other)
        squares = stat_out[p, 1] + stat_in[p, 1] + (0.5 * n_j) * (gap * gap)
        scale = lax.rsqrt(squares * (0.5 / n_j) + EPS)

        @pl.loop(0, n_j // 8)
        def _(b):
            done = [(end[b * 8 + u, i] - mean) * scale for u in range(8)]
            for u in range(8):
                std[b * 8 + u, i] = done[u]

    @pl.loop(0, n_i)
    def _(p):
        i = place(p, n_i)

        @pl.when(p < LAG)
        def _():
            pass_on(STEPS - 1, n_i - LAG + p)

        arrived(par, p)
        sent(fin, p)

        def ahead(b, total):
            parts = [advance(par, i, p, b, u) for u in range(8)]
            for u in range(8):
                end[b * 8 + u, i] = parts[u]
            while len(parts) > 1:
                parts = [a + c for a, c in zip(parts[::2], parts[1::2])]
            return total + parts[0]

        total = lax.fori_loop(0, n_j // 8, ahead, jnp.zeros((n_k, n_lev), jnp.float32))
        mean = total * (1.0 / n_j)

        def spread(b, total):
            parts = []
            for u in range(8):
                off = end[b * 8 + u, i] - mean
                parts.append(off * off)
            while len(parts) > 1:
                parts = [a + c for a, c in zip(parts[::2], parts[1::2])]
            return total + parts[0]

        stat_out[p, 0] = mean
        stat_out[p, 1] = lax.fori_loop(0, n_j // 8, spread, jnp.zeros((n_k, n_lev), jnp.float32))
        stat_copy(p).start()

    @pl.loop(0, n_i)
    def _(p):
        finish(p)

    @pl.loop(0, n_i)
    def _(p):
        sent(par, p)

        @pl.when(jnp.logical_and(passer, passed(pass_from, p)))
        def _():
            for n in (STEPS - 2, STEPS - 1):
                pass_copy(n, p).wait_send()

        stat_copy(p).wait_send()


def write_out(std, end, std_hbm, end_hbm, sem):
    parts = sem.shape[1]
    size = std.shape[0] // parts
    copies = [
        pltpu.make_async_copy(src.at[pl.ds(b * size, size)], dst.at[pl.ds(b * size, size)], sem.at[a, b])
        for b in range(parts)
        for a, (src, dst) in enumerate(((end, end_hbm), (std, std_hbm)))
    ]
    for copy in copies:
        copy.start()
    for copy in copies:
        copy.wait()


def per_device(field_values, flow_j, flow_i, flow_k):
    n_j, n_i, n_k, n_lev = sizes = field_values.shape
    f32, dma = jnp.float32, pltpu.SemaphoreType.DMA
    out = jax.ShapeDtypeStruct(sizes, f32)
    anywhere = pl.BlockSpec(memory_space=pl.ANY)
    std, end = pl.pallas_call(
        functools.partial(kernel, sizes),
        out_shape=(out, out),
        in_specs=[anywhere] * 4,
        out_specs=(pl.BlockSpec(memory_space=pltpu.VMEM),) * 2,
        scratch_shapes=[
            pltpu.VMEM((2, n_i + 2, n_j + 2, n_k, n_lev), f32),
            pltpu.VMEM((3, n_i, n_j, n_k, n_lev), f32),
            pltpu.VMEM((2, 2, n_i, n_j, n_lev), f32),
            pltpu.VMEM((2, 2, n_i, n_j, n_lev), f32),
            pltpu.VMEM((STEPS, n_i, n_j, n_lev), f32),
            pltpu.VMEM((n_i, 2, n_k, n_lev), f32),
            pltpu.VMEM((n_i, 2, n_k, n_lev), f32),
            dma((4, n_i)),
            dma((2, 2, n_i)), dma((2, 2, n_i)),
            dma((2, n_i)), dma((2, n_i)),
            dma((2, n_i)), dma((2, n_i)),
            dma((2, 2)), dma((2, 2)),
            dma((n_i,)), dma((n_i,)),
        ],
        compiler_params=pltpu.CompilerParams(
            collective_id=0, has_side_effects=True, vmem_limit_bytes=44 * 1024 * 1024
        ),
        name="transport",
    )(field_values, flow_j, flow_i, flow_k)
    return pl.pallas_call(
        write_out,
        out_shape=(out, out),
        in_specs=[pl.BlockSpec(memory_space=pltpu.VMEM)] * 2,
        out_specs=(anywhere, anywhere),
        scratch_shapes=[dma((2, 4))],
        compiler_params=pltpu.CompilerParams(vmem_limit_bytes=1024 * 1024),
        name="write_out",
    )(std, end)


def solution(mesh):
    spec = P("south", "east", "down", None)
    return jax.shard_map(
        per_device, mesh=mesh, in_specs=(spec,) * 4, out_specs=(spec, spec), check_vma=False
    )
```

```python
import functools

import jax
import jax.numpy as jnp
from jax import lax
from jax.experimental import pallas as pl
from jax.experimental.pallas import tpu as pltpu
from jax.sharding import PartitionSpec as P

STEPS = 6
RATE = 0.05
EPS = 1e-4
LAG = 1
FIRST_LAG = 2
MESH = pl.DeviceIdType.MESH


def place(p, count):
    half = lax.div(p, 2)
    return jnp.where(lax.rem(p, 2) == 0, half, count - 1 - half)


def kernel(
    sizes, x_hbm, fj_hbm, fi_hbm, fk_hbm, std, end,
    field, flows, k_out, k_in, passing, stat_out, stat_in,
    load_sem, k_send, k_recv, p_send, p_recv, j_send, j_recv, i_send, i_recv, s_send, s_recv,
):
    n_j, n_i, n_k, n_lev = sizes
    south, east, down = (lax.axis_index(a) for a in ("south", "east", "down"))
    easts, downs = lax.axis_size("east"), lax.axis_size("down")
    has = {
        "k0": down > 0, "k1": down < downs - 1,
        "i0": east > 0, "i1": east < easts - 1,
        "p0": down > 1, "p1": down < downs - 2,
    }
    near = {
        "k0": {"down": down - 1}, "k1": {"down": down + 1},
        "i0": {"east": east - 1}, "i1": {"east": east + 1},
        "p0": {"down": down - 2}, "p1": {"down": down + 2},
        "j": {"south": 1 - south},
    }
    odd = lax.rem(down, 2) == 1
    slant = (jnp.logical_and(jnp.logical_not(odd), has["k0"]), jnp.logical_and(odd, has["k1"]))

    def passed(sender, p):
        straight = lax.div(n_i * jnp.where(odd, downs - 1 - sender, sender), downs)
        shift = jnp.where(2 * straight > n_i, n_i - straight, 0)
        return lax.div((p + 1) * straight + shift, n_i) == lax.div(p * straight + shift, n_i)

    passer = jnp.where(odd, down > 1, down < downs - 2)
    pass_from = jnp.where(odd, down - 2, down + 2)
    pass_side = jnp.where(odd, 0, 1)

    def pass_copy(n, p):
        par = lax.rem(n, 2)
        return pltpu.make_async_remote_copy(
            src_ref=passing.at[n, p], dst_ref=k_in.at[par, pass_side, p],
            send_sem=p_send.at[par, p], recv_sem=k_recv.at[par, pass_side, p],
            device_id={"down": jnp.where(odd, down - 1, down + 1)}, device_id_type=MESH,
        )

    def pass_arrival(n, p):
        par = lax.rem(n, 2)
        return pltpu.make_async_remote_copy(
            src_ref=k_out.at[par, 0, p], dst_ref=passing.at[n, p],
            send_sem=p_send.at[par, p], recv_sem=p_recv.at[par, p],
            device_id={"down": pass_from}, device_id_type=MESH,
        )

    def pass_on(n, p):
        @pl.when(jnp.logical_and(passer, passed(pass_from, p)))
        def _():
            pass_arrival(n, p).wait_recv()

            @pl.when(n >= 2)
            def _():
                pass_copy(n - 2, p).wait_send()

            pass_copy(n, p).start()

    def load(a, p):
        i = place(p, n_i)
        src = (x_hbm, fj_hbm, fi_hbm, fk_hbm)[a].at[:, i]
        dst = field.at[0, i + 1, pl.ds(1, n_j)] if a == 0 else flows.at[a - 1, i]
        return pltpu.make_async_copy(src, dst, load_sem.at[a, p])

    for p in range(n_i):
        load(0, p).start()

    barrier = pltpu.get_barrier_semaphore()
    count = 1
    pl.semaphore_signal(barrier, inc=1, device_id=near["j"], device_id_type=MESH)
    for side in ("k0", "k1", "i0", "i1", "p0", "p1"):
        count = count + has[side].astype(jnp.int32)

        @pl.when(has[side])
        def _():
            pl.semaphore_signal(barrier, inc=1, device_id=near[side], device_id_type=MESH)

    def k_copy(par, d, p):
        return pltpu.make_async_remote_copy(
            src_ref=k_out.at[par, d, p], dst_ref=k_in.at[par, 1 - d, p],
            send_sem=k_send.at[par, d, p], recv_sem=k_recv.at[par, 1 - d, p],
            device_id=near[f"k{d}"], device_id_type=MESH,
        )

    def k_slant(n, d, p):
        par = lax.rem(n, 2)
        return pltpu.make_async_remote_copy(
            src_ref=k_out.at[par, d, p], dst_ref=passing.at[n, p],
            send_sem=k_send.at[par, d, p], recv_sem=p_recv.at[par, p],
            device_id=near[f"p{d}"], device_id_type=MESH,
        )

    def k_arrival(par, d, p):
        return pltpu.make_async_remote_copy(
            src_ref=k_out.at[par, 1 - d, p], dst_ref=k_in.at[par, d, p],
            send_sem=k_send.at[par, 1 - d, p], recv_sem=k_recv.at[par, d, p],
            device_id=near[f"k{d}"], device_id_type=MESH,
        )

    def j_copy(par, p):
        i = place(p, n_i)
        return pltpu.make_async_remote_copy(
            src_ref=field.at[par, i + 1, jnp.where(south == 0, n_j, 1)],
            dst_ref=field.at[par, i + 1, jnp.where(south == 0, 0, n_j + 1)],
            send_sem=j_send.at[par, p], recv_sem=j_recv.at[par, p],
            device_id=near["j"], device_id_type=MESH,
        )

    def i_copy(par, d):
        return pltpu.make_async_remote_copy(
            src_ref=field.at[par, 1 + d * (n_i - 1), pl.ds(1, n_j)],
            dst_ref=field.at[par, (1 - d) * (n_i + 1), pl.ds(1, n_j)],
            send_sem=i_send.at[par, d], recv_sem=i_recv.at[par, 1 - d],
            device_id=near[f"i{d}"], device_id_type=MESH,
        )

    def i_arrival(par, d):
        return pltpu.make_async_remote_copy(
            src_ref=field.at[par, 1 + (1 - d) * (n_i - 1), pl.ds(1, n_j)],
            dst_ref=field.at[par, d * (n_i + 1), pl.ds(1, n_j)],
            send_sem=i_send.at[par, 1 - d], recv_sem=i_recv.at[par, d],
            device_id=near[f"i{d}"], device_id_type=MESH,
        )

    rows = field.reshape(2, n_i + 2, (n_j + 2) * n_k, n_lev)

    def extract(par, p):
        i = place(p, n_i)
        for d in range(2):
            k_out[par, d, p] = rows[par, i + 1, pl.ds(n_k + d * (n_k - 1), n_j, stride=n_k), :]

    def send_slant(n, p):
        around = passed(down, p)
        for d in range(2):
            @pl.when(jnp.logical_and(slant[d], around))
            def _():
                k_slant(n, d, p).start()

    def send_rest(n, p):
        par = lax.rem(n, 2)
        around = passed(down, p)
        for d in range(2):
            @pl.when(jnp.logical_and(has[f"k{d}"], jnp.logical_not(jnp.logical_and(slant[d], around))))
            def _():
                k_copy(par, d, p).start()
        j_copy(par, p).start()
        for d in range(2):
            @pl.when(jnp.logical_and(p == d, has[f"i{d}"]))
            def _():
                i_copy(par, d).start()

    def send(n, p):
        send_slant(n, p)
        send_rest(n, p)

    def sent(par, p):
        for d in range(2):
            @pl.when(has[f"k{d}"])
            def _():
                k_copy(par, d, p).wait_send()
        j_copy(par, p).wait_send()
        for d in range(2):
            @pl.when(jnp.logical_and(p == d, has[f"i{d}"]))
            def _():
                i_copy(par, d).wait_send()

    def arrived(par, p):
        for d in range(2):
            @pl.when(has[f"k{d}"])
            def _():
                k_arrival(par, d, p).wait_recv()
        j_copy(par, p).wait_recv()
        for d in range(2):
            @pl.when(jnp.logical_and(p == d, has[f"i{d}"]))
            def _():
                i_arrival(par, d).wait_recv()

    level = lax.broadcasted_iota(jnp.int32, (n_k, n_lev), 0)
    first, last = level == 0, level == n_k - 1

    def advance(par, i, p, b, u):
        j = b * 8 + u
        mid = field[par, i + 1, j + 1]
        j0, j1 = field[par, i + 1, j], field[par, i + 1, j + 2]
        i0, i1 = field[par, i, j + 1], field[par, i + 2, j + 1]
        k0 = jnp.where(first, jnp.broadcast_to(k_in[par, 0, p, pl.ds(j, 1), :], (n_k, n_lev)), pltpu.roll(mid, 1, 0))
        k1 = jnp.where(last, jnp.broadcast_to(k_in[par, 1, p, pl.ds(j, 1), :], (n_k, n_lev)), pltpu.roll(mid, n_k - 1, 0))
        around = ((j0 + j1) + (i0 + i1)) + (k0 + k1)
        kept = (1.0 - 6.0 * RATE) * mid + RATE * around
        return kept - flows[0, i, j] * (j1 - j0) - flows[1, i, j] * (i1 - i0) - flows[2, i, j] * (k1 - k0)

    load(0, 0).wait()
    extract(0, 0)
    pl.semaphore_wait(barrier, count)
    send(0, 0)

    @pl.loop(1, n_i)
    def _(p):
        load(0, p).wait()
        extract(0, p)
        send_slant(0, p)

        @pl.when(p <= FIRST_LAG)
        def _():
            send_rest(0, p)

    @pl.loop(FIRST_LAG + 1, n_i)
    def _(p):
        pass_on(0, p - FIRST_LAG - 1)
        send_rest(0, p)

    @pl.loop(0, n_i)
    def _(p):
        for a in range(1, 4):
            load(a, p).start()

    nothing = jnp.zeros((8, n_k, n_lev), jnp.float32)
    for d in range(2):
        @pl.when(jnp.logical_not(has[f"k{d}"]))
        def _():
            @pl.loop(0, 2 * n_i)
            def _(q):
                k_in[lax.div(q, n_i), d, lax.rem(q, n_i)] = jnp.zeros((n_j, n_lev), jnp.float32)

        @pl.when(jnp.logical_not(has[f"i{d}"]))
        def _():
            @pl.loop(0, n_j // 8)
            def _(b):
                for par in range(2):
                    field[par, d * (n_i + 1), pl.ds(1 + b * 8, 8)] = nothing

        @pl.when(south == d)
        def _():
            @pl.loop(0, n_i)
            def _(i):
                for par in range(2):
                    field[par, i + 1, d * (n_j + 1)] = nothing[0]

    @pl.loop(n_i - FIRST_LAG - 1, n_i - LAG)
    def _(p):
        pass_on(0, p)

    @pl.loop(0, STEPS - 1)
    def _(n):
        par = lax.rem(n, 2)

        @pl.loop(0, n_i)
        def _(p):
            i = place(p, n_i)

            @pl.when(n == 0)
            def _():
                for a in range(1, 4):
                    load(a, p).wait()

            arrived(par, p)

            @pl.when(n > 0)
            def _():
                sent(1 - par, p)

            @pl.loop(0, n_j // 8)
            def _(b):
                new = [advance(par, i, p, b, u) for u in range(8)]
                for u in range(8):
                    field[1 - par, i + 1, b * 8 + u + 1] = new[u]

            extract(1 - par, p)
            at = (n + 1) * n_i + p - LAG
            pass_on(lax.div(at, n_i), lax.rem(at, n_i))
            send(n + 1, p)

    par = (STEPS - 1) % 2
    fin = 1 - par

    def stat_copy(p):
        return pltpu.make_async_remote_copy(
            src_ref=stat_out.at[p], dst_ref=stat_in.at[p],
            send_sem=s_send.at[p], recv_sem=s_recv.at[p],
            device_id=near["j"], device_id_type=MESH,
        )

    def finish(p):
        i = place(p, n_i)
        stat_copy(p).wait_recv()
        mine, other = stat_out[p, 0], stat_in[p, 0]
        gap = mine - other
        mean = 0.5 * (mine + other)
        squares = stat_out[p, 1] + stat_in[p, 1] + (0.5 * n_j) * (gap * gap)
        scale = lax.rsqrt(squares * (0.5 / n_j) + EPS)

        @pl.loop(0, n_j // 8)
        def _(b):
            done = [(end[b * 8 + u, i] - mean) * scale for u in range(8)]
            for u in range(8):
                std[b * 8 + u, i] = done[u]

    @pl.loop(0, n_i)
    def _(p):
        i = place(p, n_i)

        @pl.when(p < LAG)
        def _():
            pass_on(STEPS - 1, n_i - LAG + p)

        arrived(par, p)
        sent(fin, p)

        def ahead(b, total):
            parts = [advance(par, i, p, b, u) for u in range(8)]
            for u in range(8):
                end[b * 8 + u, i] = parts[u]
            while len(parts) > 1:
                parts = [a + c for a, c in zip(parts[::2], parts[1::2])]
            return total + parts[0]

        total = lax.fori_loop(0, n_j // 8, ahead, jnp.zeros((n_k, n_lev), jnp.float32))
        mean = total * (1.0 / n_j)

        def spread(b, total):
            parts = []
            for u in range(8):
                off = end[b * 8 + u, i] - mean
                parts.append(off * off)
            while len(parts) > 1:
                parts = [a + c for a, c in zip(parts[::2], parts[1::2])]
            return total + parts[0]

        stat_out[p, 0] = mean
        stat_out[p, 1] = lax.fori_loop(0, n_j // 8, spread, jnp.zeros((n_k, n_lev), jnp.float32))
        stat_copy(p).start()

    @pl.loop(0, n_i)
    def _(p):
        finish(p)

    @pl.loop(0, n_i)
    def _(p):
        sent(par, p)

        @pl.when(jnp.logical_and(passer, passed(pass_from, p)))
        def _():
            for n in (STEPS - 2, STEPS - 1):
                pass_copy(n, p).wait_send()

        stat_copy(p).wait_send()


def write_out(std, end, std_hbm, end_hbm, sem):
    parts = sem.shape[1]
    size = std.shape[0] // parts
    copies = [
        pltpu.make_async_copy(src.at[pl.ds(b * size, size)], dst.at[pl.ds(b * size, size)], sem.at[a, b])
        for b in range(parts)
        for a, (src, dst) in enumerate(((end, end_hbm), (std, std_hbm)))
    ]
    for copy in copies:
        copy.start()
    for copy in copies:
        copy.wait()


def per_device(field_values, flow_j, flow_i, flow_k):
    n_j, n_i, n_k, n_lev = sizes = field_values.shape
    f32, dma = jnp.float32, pltpu.SemaphoreType.DMA
    out = jax.ShapeDtypeStruct(sizes, f32)
    anywhere = pl.BlockSpec(memory_space=pl.ANY)
    std, end = pl.pallas_call(
        functools.partial(kernel, sizes),
        out_shape=(out, out),
        in_specs=[anywhere] * 4,
        out_specs=(pl.BlockSpec(memory_space=pltpu.VMEM),) * 2,
        scratch_shapes=[
            pltpu.VMEM((2, n_i + 2, n_j + 2, n_k, n_lev), f32),
            pltpu.VMEM((3, n_i, n_j, n_k, n_lev), f32),
            pltpu.VMEM((2, 2, n_i, n_j, n_lev), f32),
            pltpu.VMEM((2, 2, n_i, n_j, n_lev), f32),
            pltpu.VMEM((STEPS, n_i, n_j, n_lev), f32),
            pltpu.VMEM((n_i, 2, n_k, n_lev), f32),
            pltpu.VMEM((n_i, 2, n_k, n_lev), f32),
            dma((4, n_i)),
            dma((2, 2, n_i)), dma((2, 2, n_i)),
            dma((2, n_i)), dma((2, n_i)),
            dma((2, n_i)), dma((2, n_i)),
            dma((2, 2)), dma((2, 2)),
            dma((n_i,)), dma((n_i,)),
        ],
        compiler_params=pltpu.CompilerParams(
            collective_id=0, has_side_effects=True, vmem_limit_bytes=44 * 1024 * 1024
        ),
        name="transport",
    )(field_values, flow_j, flow_i, flow_k)
    return pl.pallas_call(
        write_out,
        out_shape=(out, out),
        in_specs=[pl.BlockSpec(memory_space=pltpu.VMEM)] * 2,
        out_specs=(anywhere, anywhere),
        scratch_shapes=[dma((2, 4))],
        compiler_params=pltpu.CompilerParams(vmem_limit_bytes=1024 * 1024),
        name="write_out",
    )(std, end)


def solution(mesh):
    spec = P("south", "east", "down", None)
    return jax.shard_map(
        per_device, mesh=mesh, in_specs=(spec,) * 4, out_specs=(spec, spec), check_vma=False
    )
```
